32 devices in a mesh: seq: 2 (over x), fsdp: 16 (over z, y, core).
Axes of the slice: x: 2, y: 2, z: 4, core: 2. Of those that a mesh axis runs over, the one named last changes fastest.
Arguments:
- tokens: bfloat16 [16, 256, 2048], P('fsdp', 'seq'), may hold values from -6 to 6
- token_ids: int32 [16, 256], P('fsdp', 'seq'), may hold values from 0 to 11, as said below
- norm_gain: float32 [2048], replicated, may hold values from 0.1 to 1.9
- w_in: bfloat16 [2048, 2048], P('fsdp'), may hold values from -0.125 to 0.125
- rates: float32 [1024], replicated, may hold values from 1.953125e-05 to 0.034
- phases: float32 [1024], replicated, may hold values from 0 to 0.6
- forget: float32 [1024], replicated, may hold values from 0.2 to 0.5
- readout: float32 [2, 1024], replicated, may hold values from -3 to 3
- skip: float32 [2048], replicated, may hold values from -1 to 1
- out_grad: bfloat16 [16, 256, 2048], P('fsdp', 'seq'), may hold values from -0.09375 to 0.09375
Outputs:
- mixed: bfloat16 [16, 256, 2048], P('fsdp', 'seq')
- grad_w_in: float32 [2048, 2048], P('fsdp', 'seq')
The draws below stay inside these ranges and needn't reach their ends.
Inputs may be any that keep to these rules, and one draw needn't show every extreme that they name: `token_ids`: ids 0 to 3 are the four bases; higher ids are special tokens.
All inputs are finite; a program needn't handle non-finite values.
Results may differ from the reference program's by a relative error of at most 0.01.
Values may be sent and summed in bfloat16 or wider, within the bound.
No kernel may reach another device: no remote copies, remote signals or barrier semaphores. Data moves between devices by JAX's collectives and lax.ppermute only.
A program may use at most 128 MiB of HBM per device.

```python
import jax
import jax.numpy as jnp
from jax import lax

D = 2048
PAIRS = 1024
VOCAB = 12
TOK_DEV = 128
SEQS = 16
LEN = 256
N_SEQ = 2
N_FSDP = 16


def draw_token_ids(key, part):
    first_key, second_key, third_key = jax.random.split(jax.random.fold_in(key, 11), 3)
    bases = jax.random.randint(first_key, (SEQS, LEN), 0, 4)
    marked = jax.random.randint(second_key, (SEQS, LEN), 0, LEN) < 2
    specials = jax.random.randint(third_key, (SEQS, LEN), 4, VOCAB)
    return jnp.where(marked, specials, bases).astype(jnp.int32)


def draw_rates(key, part):
    lowest = 0.005 / LEN
    highest = 1.0 / 30.0
    fraction = jax.random.uniform(jax.random.fold_in(key, 23), (PAIRS,), jnp.float32)
    low_log = jnp.log(jnp.float32(lowest))
    high_log = jnp.log(jnp.float32(highest))
    return jnp.exp(low_log + fraction * (high_log - low_log)).astype(jnp.float32)


def levels(own_key, shape, shards, smallest, largest):
    loudness = 1.0
    for position, blocks in shards:
        draws = jax.random.uniform(jax.random.fold_in(jax.random.fold_in(own_key, 6), position), (blocks,), jnp.float32, smallest / len(shards), largest / len(shards))
        loudness = loudness * jnp.repeat(jnp.exp(draws), shape[position] // blocks).reshape((-1,) + (1,) * (len(shape) - 1 - position))
    return loudness


def centred(stream_key, shape, deviation, bound, cuts=(), kind=jnp.bfloat16):
    result = deviation * jax.random.normal(stream_key, shape, jnp.float32)
    if cuts:
        result = result * levels(stream_key, shape, cuts, -0.22, 0.18)
    return jnp.clip(result, -bound, bound).astype(kind)


def setup_inputs(seed: int = 0) -> dict:
    splits = jax.random.split(jax.random.key(seed), 11)
    tokens = centred(splits[0], (SEQS, LEN, D), 1.0, 6.0, ((0, 16), (1, 2)))
    token_ids = draw_token_ids(jax.random.fold_in(splits[10], 71), 0)
    norm_gain = jnp.clip(1.0 + 0.18 * jax.random.normal(splits[2], (D,), jnp.float32), 0.1, 1.9)
    w_in = centred(splits[3], (D, 2 * PAIRS), D ** -0.5, 0.125, ((0, 16),))
    rates = draw_rates(jax.random.fold_in(splits[10], 71), 0)
    phases = jnp.clip(jax.random.uniform(splits[5], (PAIRS,), jnp.float32, 0.0, 0.6), 0.0, 0.6)
    forget = jnp.clip(jax.random.uniform(splits[6], (PAIRS,), jnp.float32, 0.2, 0.5), 0.2, 0.5)
    readout = centred(splits[7], (2, PAIRS), 1.0, 3.0, (), jnp.float32)
    skip = jnp.clip(jax.random.uniform(splits[8], (D,), jnp.float32, -1.0, 1.0), -1.0, 1.0)
    out_grad = centred(splits[9], (SEQS, LEN, D), (TOK_DEV * N_SEQ * N_FSDP) ** -0.5, 0.09375, ((0, 16), (1, 2)))
    return dict(tokens=tokens, token_ids=token_ids, norm_gain=norm_gain, w_in=w_in, rates=rates, phases=phases, forget=forget, readout=readout, skip=skip, out_grad=out_grad)


epsilon = 1e-06
first_special = 4

def chain_join(earlier, later):
    a_re, a_im, b_re, b_im, c_re, c_im = earlier
    p_re, p_im, q_re, q_im, s_re, s_im = later
    return (p_re * a_re - p_im * a_im, p_re * a_im + p_im * a_re, p_re * b_re - p_im * b_im + q_re, p_re * b_im + p_im * b_re + q_im, p_re * c_re + p_im * c_im + s_re, p_re * c_im - p_im * c_re + s_im)

def reference(tokens, token_ids, norm_gain, w_in, rates, phases, forget, readout, skip, out_grad):
    pairs = rates.shape[0]
    radius = jnp.exp(-rates)
    in_scale = jnp.sqrt(-jnp.expm1(-2.0 * rates))
    up_re = readout[0]
    up_im = readout[1]

    def one_sequence(total, members):
        block_in, block_ids, block_grad = members
        widened = block_in.astype(jnp.float32)
        spread = lax.optimization_barrier(jnp.mean(widened * widened, axis=1, keepdims=True))
        normed = (widened * lax.rsqrt(spread + epsilon) * norm_gain).astype(jnp.bfloat16)
        inputs = jnp.dot(normed, w_in, preferred_element_type=jnp.float32)
        retain = jnp.where(block_ids[:, None] >= first_special, 1.0 - forget[None, :], 1.0)
        decay_re = retain * radius * jnp.cos(phases)
        decay_im = retain * radius * jnp.sin(phases)
        drive_re = in_scale * inputs[:, :pairs]
        drive_im = in_scale * inputs[:, pairs:]
        grad_wide = block_grad.astype(jnp.float32)
        state_re = up_re * grad_wide[:, :pairs] + up_im * grad_wide[:, pairs:]
        state_im = up_re * grad_wide[:, pairs:] - up_im * grad_wide[:, :pairs]
        back_re = decay_re * state_re + decay_im * state_im
        back_im = decay_re * state_im - decay_im * state_re
        elements = (decay_re, decay_im, drive_re, drive_im, back_re, back_im)
        ahead = lax.associative_scan(chain_join, elements, axis=0)
        behind = lax.associative_scan(chain_join, elements, reverse=True, axis=0)
        sum_re = ahead[2] + behind[2]
        sum_im = ahead[3] + behind[3]
        out_re = up_re * sum_re - up_im * sum_im
        out_im = up_re * sum_im + up_im * sum_re
        branch = jnp.concatenate([out_re, out_im], axis=1)
        mixed = (widened + branch + skip * normed.astype(jnp.float32)).astype(jnp.bfloat16)
        zero_row = jnp.zeros((1, pairs), jnp.float32)
        later_re = jnp.concatenate([behind[4][1:], zero_row], axis=0)
        later_im = jnp.concatenate([behind[5][1:], zero_row], axis=0)
        former_re = jnp.concatenate([zero_row, ahead[4][:-1]], axis=0)
        former_im = jnp.concatenate([zero_row, ahead[5][:-1]], axis=0)
        grad_re = in_scale * (2.0 * state_re + later_re + former_re)
        grad_im = in_scale * (2.0 * state_im + later_im + former_im)
        input_grad = jnp.concatenate([grad_re, grad_im], axis=1).astype(jnp.bfloat16)
        total = total + lax.dot_general(normed, input_grad, (((0,), (0,)), ((), ())), preferred_element_type=jnp.float32)
        return (total, mixed)
    start = jnp.zeros((w_in.shape[0], w_in.shape[1]), jnp.float32)
    grad_w_in, mixed = lax.scan(one_sequence, start, (tokens, token_ids, out_grad))
    return (mixed, grad_w_in)
```

```python
import functools

import jax
import jax.numpy as jnp
from jax import lax
from jax.experimental import pallas as pl
from jax.experimental.pallas import tpu as pltpu
from jax.sharding import Mesh, PartitionSpec as P

epsilon = 1e-06
first_special = 4
ROWS = 8
BF16 = jnp.bfloat16
F32 = jnp.float32


def carried_in(value, axis, join, neutral, backward):
    count, mine = (lax.axis_size(axis), lax.axis_index(axis))
    pieces = jax.tree.map(lambda part: lax.all_gather(part, axis), value)
    if backward:
        pieces = jax.tree.map(lambda part: part[::-1], pieces)
        mine = count - 1 - mine
    running = jax.tree.map(
        lambda part, zero: jnp.full_like(part, 0) + jnp.asarray(zero, part.dtype), value, neutral
    )

    def turn(position, running):
        longer = join(running, jax.tree.map(lambda part: part[position], pieces))
        return jax.tree.map(lambda new, old: jnp.where(position < mine, new, old), longer, running)

    return lax.fori_loop(0, count - 1, turn, running)


def chain_join(earlier, later):
    a_re, a_im, b_re, b_im, c_re, c_im = earlier
    p_re, p_im, q_re, q_im, s_re, s_im = later
    return (
        p_re * a_re - p_im * a_im,
        p_re * a_im + p_im * a_re,
        p_re * b_re - p_im * b_im + q_re,
        p_re * b_im + p_im * b_re + q_im,
        p_re * c_re + p_im * c_im + s_re,
        p_re * c_im - p_im * c_re + s_im,
    )


def apply_carry(local, carry):
    prod_re, prod_im, state_re, state_im, adjoint_re, adjoint_im = local
    enter_re = carry[2][None, :]
    enter_im = carry[3][None, :]
    back_enter_re = carry[4][None, :]
    back_enter_im = carry[5][None, :]
    state_re = state_re + prod_re * enter_re - prod_im * enter_im
    state_im = state_im + prod_re * enter_im + prod_im * enter_re
    adjoint_re = adjoint_re + prod_re * back_enter_re + prod_im * back_enter_im
    adjoint_im = adjoint_im + prod_re * back_enter_im - prod_im * back_enter_re
    return (state_re, state_im, adjoint_re, adjoint_im)


def rms_normed(block_in, norm_gain):
    widened = block_in.astype(F32)
    spread = jnp.mean(widened * widened, axis=1, keepdims=True)
    return widened, (widened * lax.rsqrt(spread + epsilon) * norm_gain).astype(BF16)


def body_any(tokens, token_ids, norm_gain, w_in, rates, phases, forget, readout, skip, out_grad):
    block_ids = token_ids[0]
    block_grad = out_grad[0]
    pairs = rates.shape[0]
    widened, normed = rms_normed(tokens[0], norm_gain)
    inputs = jnp.dot(
        normed, lax.all_gather(w_in, "fsdp", axis=0, tiled=True), preferred_element_type=F32
    )
    radius = jnp.exp(-rates)
    in_scale = jnp.sqrt(-jnp.expm1(-2.0 * rates))
    up_re = readout[0]
    up_im = readout[1]
    retain = jnp.where(block_ids[:, None] >= first_special, 1.0 - forget[None, :], 1.0)
    decay_re = retain * radius * jnp.cos(phases)
    decay_im = retain * radius * jnp.sin(phases)
    drive_re = in_scale * inputs[:, :pairs]
    drive_im = in_scale * inputs[:, pairs:]
    grad_wide = block_grad.astype(F32)
    state_re = up_re * grad_wide[:, :pairs] + up_im * grad_wide[:, pairs:]
    state_im = up_re * grad_wide[:, pairs:] - up_im * grad_wide[:, :pairs]
    back_re = decay_re * state_re + decay_im * state_im
    back_im = decay_re * state_im - decay_im * state_re
    elements = (decay_re, decay_im, drive_re, drive_im, back_re, back_im)
    ahead = lax.associative_scan(chain_join, elements, axis=0)
    behind = lax.associative_scan(chain_join, elements, reverse=True, axis=0)
    ahead_summary = tuple((member[-1] for member in ahead))
    behind_summary = tuple((member[0] for member in behind))
    ones_row = jnp.ones((pairs,), F32)
    zeros_row = jnp.zeros((pairs,), F32)
    identity = (ones_row, zeros_row, zeros_row, zeros_row, zeros_row, zeros_row)
    ahead_in = carried_in(ahead_summary, "seq", chain_join, identity, False)
    behind_in = carried_in(behind_summary, "seq", chain_join, identity, True)
    fwd_re, fwd_im, sigma_re, sigma_im = apply_carry(ahead, ahead_in)
    bwd_re, bwd_im, rho_re, rho_im = apply_carry(behind, behind_in)
    sum_re = fwd_re + bwd_re
    sum_im = fwd_im + bwd_im
    out_re = up_re * sum_re - up_im * sum_im
    out_im = up_re * sum_im + up_im * sum_re
    branch = jnp.concatenate([out_re, out_im], axis=1)
    mixed = (widened + branch + skip * normed.astype(F32)).astype(BF16)
    later_re = jnp.concatenate([rho_re[1:], behind_in[4][None, :]], axis=0)
    later_im = jnp.concatenate([rho_im[1:], behind_in[5][None, :]], axis=0)
    former_re = jnp.concatenate([ahead_in[4][None, :], sigma_re[:-1]], axis=0)
    former_im = jnp.concatenate([ahead_in[5][None, :], sigma_im[:-1]], axis=0)
    grad_re = in_scale * (2.0 * state_re + later_re + former_re)
    grad_im = in_scale * (2.0 * state_im + later_im + former_im)
    input_grad = jnp.concatenate([grad_re, grad_im], axis=1).astype(BF16)
    row_block = lax.psum_scatter(
        lax.dot_general(
            normed, input_grad, (((0,), (0,)), ((), ())), preferred_element_type=F32
        ),
        "fsdp",
        scatter_dimension=0,
        tiled=True,
    )
    grad_w_in = lax.psum_scatter(row_block, "seq", scatter_dimension=1, tiled=True)
    return (mixed[None], grad_w_in)


SLAB = ("x", "y", "c")
FLIPS = [(dx, dy, dc) for dx in (0, 1) for dy in (0, 1) for dc in (0, 1)]


def flip(value, *axes):
    count = 2 ** len(axes)
    return lax.ppermute(value, axes, [(i, count - 1 - i) for i in range(count)])


def z_flip(value, distance, count):
    return lax.ppermute(value, "z", [(i, i ^ distance) for i in range(count)])


def cmul(a_re, a_im, b_re, b_im):
    return a_re * b_re - a_im * b_im, a_re * b_im + a_im * b_re


def enter_chunks(x_re, x_im, p_re, p_im, backward):
    rows = lax.broadcasted_iota(jnp.int32, x_re.shape, 0)

    def moved(value, by, fill):
        if backward:
            return jnp.where(rows < ROWS - by, pltpu.roll(value, ROWS - by, 0), fill)
        return jnp.where(rows >= by, pltpu.roll(value, by, 0), fill)

    by = 1
    while by < ROWS:
        from_re, from_im = moved(x_re, by, 0.0), moved(x_im, by, 0.0)
        add_re, add_im = cmul(p_re, p_im, from_re, from_im)
        if 2 * by < ROWS:
            p_re, p_im = cmul(p_re, p_im, moved(p_re, by, 1.0), moved(p_im, by, 0.0))
        x_re, x_im = x_re + add_re, x_im + add_im
        by *= 2
    return moved(x_re, 1, 0.0), moved(x_im, 1, 0.0)


def both_ways(adjoint, count, steps, pars, keep, val_re, val_im, up, down):
    wide = val_re.shape[-1]
    lam_re = jnp.broadcast_to(pars[0:1, :], (ROWS, wide))
    lam_im = jnp.broadcast_to(pars[1:2, :], (ROWS, wide))
    if adjoint:
        lam_im = -lam_im

    def load(q, j):
        at = pl.ds(j, ROWS, stride=steps)
        return val_re[q, at, :], val_im[q, at, :]

    def step(q, j, state):
        v_re, v_im = load(q, j)
        held = keep[q, j]
        if adjoint:
            out_re, out_im = v_re + state[0], v_im + state[1]
            n_re, n_im = cmul(lam_re, lam_im, out_re, out_im)
            return (held * n_re, held * n_im), (out_re, out_im)
        n_re, n_im = cmul(lam_re, lam_im, held * state[0], held * state[1])
        n_re, n_im = n_re + v_re, n_im + v_im
        return (n_re, n_im), (n_re, n_im)

    zero = jnp.zeros((ROWS, wide), F32)

    def first(i, carry):
        result = []
        for q in range(count):
            ahead, behind, kept = carry[q]
            ahead, _ = step(q, i, ahead)
            behind, _ = step(q, steps - 1 - i, behind)
            result.append((ahead, behind, kept * keep[q, i]))
        return tuple(result)

    start = tuple(((zero, zero), (zero, zero), zero + 1.0) for _ in range(count))
    ends = lax.fori_loop(0, steps, first, start, unroll=2)
    pow_re, pow_im = lam_re, lam_im
    done = 1
    while done < steps:
        pow_re, pow_im = cmul(pow_re, pow_im, pow_re, pow_im)
        done *= 2
    enters = []
    for ahead, behind, kept in ends:
        p_re, p_im = kept * pow_re, kept * pow_im
        enters.append(
            (enter_chunks(*ahead, p_re, p_im, False), enter_chunks(*behind, p_re, p_im, True))
        )

    def second(i, carry):
        result = []
        for q in range(count):
            ahead, behind = carry[q]
            ahead, out = step(q, i, ahead)
            up[0, q, i] = out[0]
            up[1, q, i] = out[1]
            behind, out = step(q, steps - 1 - i, behind)
            down[0, q, steps - 1 - i] = out[0]
            down[1, q, steps - 1 - i] = out[1]
            result.append((ahead, behind))
        return tuple(result)

    lax.fori_loop(0, steps, second, tuple(enters), unroll=2)


def fill_keep(count, steps, flags, pars, keep):
    lose = jnp.broadcast_to(pars[2:3, :], keep.shape[-2:])
    for q in range(count):
        chunk = flags[q]
        for j in range(steps):
            keep[q, j] = 1.0 - jnp.broadcast_to(chunk[:, j : j + 1], lose.shape) * lose


def adjoint_kernel(count, steps, og, flags, pars, ig, val_re, val_im, keep, up, down):
    wide = val_re.shape[-1]
    half = og.shape[1]
    c_re, c_im = pars[3:4, :], pars[4:5, :]
    for m in range(2 * count):
        x, q = divmod(m, count)
        q_re = og[m, :, :wide].astype(F32)
        q_im = og[m, :, wide:].astype(F32)
        rows = pl.ds(x * half, half)
        val_re[q, rows, :] = c_re * q_re + c_im * q_im
        val_im[q, rows, :] = c_re * q_im - c_im * q_re
    fill_keep(count, steps, flags, pars, keep)
    both_ways(True, count, steps, pars, keep, val_re, val_im, up, down)
    per = half // steps
    for m in range(2 * count):
        x, q = divmod(m, count)
        for s in range(per):
            row = x * per + s
            for part in range(2):
                total = up[part, q, :, row, :] + down[part, q, :, row, :]
                ig[m, s * steps : (s + 1) * steps, part * wide : (part + 1) * wide] = total.astype(BF16)


def forward_kernel(count, steps, layout, *refs):
    nbs, refs = refs[: 2 * count], refs[2 * count :]
    wbs, refs = refs[: layout["z"]], refs[layout["z"] :]
    flags, pars, branch, w_all, val_re, val_im, keep, up, down = refs
    wide = val_re.shape[-1]
    half = nbs[0].shape[0]
    here = {axis: lax.axis_index(axis) for axis in ("x", "z", "y", "c")}
    depth = w_all.shape[0] // (layout["z"] * count)
    for dz in range(layout["z"]):
        for d in range(count):
            dy, dc = divmod(d, 2)
            block = ((here["z"] ^ dz) * 2 + (here["y"] ^ dy)) * 2 + (here["c"] ^ dc)
            at = pl.multiple_of(block * depth, depth)
            w_all[pl.ds(at, depth), :] = wbs[dz][d]
    fill_keep(count, steps, flags, pars, keep)
    for k, (dx, dy, dc) in enumerate(FLIPS):
        got = jnp.dot(nbs[k][...], w_all[...], preferred_element_type=F32)
        q = (here["y"] ^ dy) * 2 + (here["c"] ^ dc)
        rows = pl.ds(pl.multiple_of((here["x"] ^ dx) * half, half), half)
        val_re[q, rows, :] = got[:, :wide]
        val_im[q, rows, :] = got[:, wide:]
    both_ways(False, count, steps, pars, keep, val_re, val_im, up, down)
    c_re, c_im = pars[3:4, :], pars[4:5, :]
    per = half // steps
    for m in range(2 * count):
        x, q = divmod(m, count)
        for s in range(per):
            row = x * per + s
            s_re = up[0, q, :, row, :] + down[0, q, :, row, :]
            s_im = up[1, q, :, row, :] + down[1, q, :, row, :]
            rows = pl.ds(s * steps, steps)
            branch[m, rows, :wide] = (c_re * s_re - c_im * s_im).astype(BF16)
            branch[m, rows, wide:] = (c_re * s_im + c_im * s_re).astype(BF16)


def outer_kernel(count, layout, *refs):
    nbs, refs = refs[: 2 * count], refs[2 * count :]
    ig, outs = refs[0], refs[1:]
    here = {axis: lax.axis_index(axis) for axis in ("x", "z", "y", "c")}
    across = outs[0].shape[1]
    for dz, out in enumerate(outs):
        columns = pl.ds(pl.multiple_of((here["z"] ^ dz) * across, across), across)
        total = jnp.zeros(out.shape, F32)
        for k, (dx, dy, dc) in enumerate(FLIPS):
            m = ((here["x"] ^ dx) * 2 + (here["y"] ^ dy)) * 2 + (here["c"] ^ dc)
            total += lax.dot_general(
                ig[m], nbs[k][:, columns], (((0,), (0,)), ((), ())), preferred_element_type=F32
            )
        out[...] = total.astype(out.dtype)


def scan_scratch(count, steps, wide):
    return [
        pltpu.VMEM((count, ROWS * steps, wide), F32),
        pltpu.VMEM((count, ROWS * steps, wide), F32),
        pltpu.VMEM((count, steps, ROWS, wide), F32),
        pltpu.VMEM((2, count, steps, ROWS, wide), F32),
        pltpu.VMEM((2, count, steps, ROWS, wide), F32),
    ]


def whole_refs(n):
    return [pl.BlockSpec(memory_space=pltpu.VMEM)] * n


def body_slab(layout, tokens, token_ids, norm_gain, w_in, rates, phases, forget, readout, skip, out_grad):
    half = tokens.shape[1]
    model = tokens.shape[2]
    pairs = rates.shape[0]
    n_z = layout["z"]
    count = 4
    members = 2 * count
    wide = pairs // members
    steps = 2 * half // ROWS
    mine = (lax.axis_index("x") * 2 + lax.axis_index("y")) * 2 + lax.axis_index("c")
    params = pltpu.CompilerParams(vmem_limit_bytes=56 * 2**20)

    widened, normed = rms_normed(tokens[0], norm_gain)
    cut = half // 2
    n_x = flip(normed, "x")
    n_y = flip(normed, "y")
    n_c = flip(normed, "c")
    n_xy = jnp.concatenate([flip(n_y[:cut], "x"), flip(n_x[cut:], "y")], axis=0)
    n_xc = flip(n_x, "c")
    n_yc = flip(n_y, "c")
    n_xyc = flip(n_xy, "c")
    nbs = [normed, n_c, n_y, n_yc, n_x, n_xc, n_xy, n_xyc]

    w_cut = w_in.reshape(w_in.shape[0], 2, members, wide)
    w_rel = []
    for dy, dc in ((0, 0), (0, 1), (1, 0), (1, 1)):
        to = (lax.axis_index("x") * 2 + (lax.axis_index("y") ^ dy)) * 2 + (lax.axis_index("c") ^ dc)
        piece = lax.dynamic_index_in_dim(w_cut, to, 2, keepdims=False).reshape(-1, 2 * wide)
        axes = tuple(name for name, on in (("y", dy), ("c", dc)) if on)
        w_rel.append(flip(piece, *axes) if axes else piece)
    w_own = jnp.stack(w_rel)
    w_2 = z_flip(w_own, 2, n_z)
    w_1 = z_flip(w_own, 1, n_z)
    w_3 = z_flip(w_2, 1, n_z)

    ids = lax.all_gather(token_ids[0], SLAB, axis=0).reshape(2, count, half)
    flags = jnp.where(ids >= first_special, 1.0, 0.0).astype(F32)
    flags = flags.transpose(1, 0, 2).reshape(count, ROWS, steps)

    radius = jnp.exp(-rates)
    in_scale = jnp.sqrt(-jnp.expm1(-2.0 * rates))
    rows = [radius * jnp.cos(phases), radius * jnp.sin(phases), forget, in_scale * readout[0], in_scale * readout[1]]
    rows = jnp.stack(rows + [jnp.zeros_like(rates)] * (ROWS - len(rows)))
    pars = lax.dynamic_slice_in_dim(rows, mine * wide, wide, axis=1)

    og = out_grad[0].reshape(half, 2, members, wide).transpose(2, 0, 1, 3).reshape(members, half, 2 * wide)
    og = lax.all_to_all(og, SLAB, 0, 0, tiled=True)

    ig = pl.pallas_call(
        functools.partial(adjoint_kernel, count, steps),
        out_shape=jax.ShapeDtypeStruct((members, half, 2 * wide), BF16),
        in_specs=whole_refs(3),
        out_specs=pl.BlockSpec(memory_space=pltpu.VMEM),
        scratch_shapes=scan_scratch(count, steps, wide),
        compiler_params=params,
        cost_estimate=pl.CostEstimate(flops=4_000_000, bytes_accessed=2_000_000, transcendentals=0),
        name="adjoint",
    )(og, flags, pars)

    across = model // n_z
    parts = pl.pallas_call(
        functools.partial(outer_kernel, count, layout),
        out_shape=[jax.ShapeDtypeStruct((2 * wide, across), BF16 if dz else F32) for dz in range(n_z)],
        in_specs=whole_refs(members + 1),
        out_specs=whole_refs(n_z),
        compiler_params=params,
        cost_estimate=pl.CostEstimate(flops=2 * members * half * model * 2 * wide, bytes_accessed=6_000_000, transcendentals=0),
        name="outer",
    )(*nbs, ig)
    total = parts[0]
    for dz in range(1, n_z):
        total = total + z_flip(parts[dz], dz, n_z).astype(F32)

    branch = pl.pallas_call(
        functools.partial(forward_kernel, count, steps, layout),
        out_shape=jax.ShapeDtypeStruct((members, half, 2 * wide), BF16),
        in_specs=whole_refs(members + n_z + 2),
        out_specs=pl.BlockSpec(memory_space=pltpu.VMEM),
        scratch_shapes=[pltpu.VMEM((model, 2 * wide), BF16)] + scan_scratch(count, steps, wide),
        compiler_params=params,
        cost_estimate=pl.CostEstimate(flops=2 * members * half * model * 2 * wide, bytes_accessed=6_000_000, transcendentals=0),
        name="forward",
    )(*nbs, w_own, w_1, w_2, w_3, flags, pars)
    branch = lax.all_to_all(branch, SLAB, 0, 0, tiled=True)
    branch = branch.reshape(members, half, 2, wide).transpose(1, 2, 0, 3).reshape(half, model)
    mixed = (widened + branch.astype(F32) + skip * normed.astype(F32)).astype(BF16)

    total = total.astype(BF16).reshape(2, wide, count, across // count).transpose(0, 2, 1, 3)
    total = total.reshape(members, wide, across // count)
    total = lax.all_to_all(total, SLAB, 0, 0, tiled=True)
    grad_w_in = total.reshape(pairs, across // count).astype(F32).T
    return (mixed[None], grad_w_in)


def solution(mesh):
    n_seq, n_fsdp = mesh.shape["seq"], mesh.shape["fsdp"]
    if n_seq == 2 and n_fsdp == 16:
        layout = {"x": n_seq, "z": n_fsdp // 4, "y": 2, "c": 2}
        mesh = Mesh(mesh.devices.reshape(tuple(layout.values())), tuple(layout))
        body, fsdp, seq = functools.partial(body_slab, layout), ("z", "y", "c"), "x"
    else:
        body, fsdp, seq = body_any, "fsdp", "seq"
    in_specs = (
        P(fsdp, seq, None),
        P(fsdp, seq),
        P(),
        P(fsdp, None),
        P(),
        P(),
        P(),
        P(),
        P(),
        P(fsdp, seq, None),
    )
    out_specs = (P(fsdp, seq, None), P(fsdp, seq))
    return jax.shard_map(body, mesh=mesh, in_specs=in_specs, out_specs=out_specs, check_vma=False)
```

```python
import functools

import jax
import jax.numpy as jnp
from jax import lax
from jax.experimental import pallas as pl
from jax.experimental.pallas import tpu as pltpu
from jax.sharding import Mesh, PartitionSpec as P


epsilon = 1e-06
first_special = 4
ROWS = 8
BF16 = jnp.bfloat16
F32 = jnp.float32


def carried_in(value, axis, join, neutral, backward):
    count, mine = (lax.axis_size(axis), lax.axis_index(axis))
    pieces = jax.tree.map(lambda part: lax.all_gather(part, axis), value)
    if backward:
        pieces = jax.tree.map(lambda part: part[::-1], pieces)
        mine = count - 1 - mine
    running = jax.tree.map(
        lambda part, zero: jnp.full_like(part, 0) + jnp.asarray(zero, part.dtype), value, neutral
    )

    def turn(position, running):
        longer = join(running, jax.tree.map(lambda part: part[position], pieces))
        return jax.tree.map(lambda new, old: jnp.where(position < mine, new, old), longer, running)

    return lax.fori_loop(0, count - 1, turn, running)


def chain_join(earlier, later):
    a_re, a_im, b_re, b_im, c_re, c_im = earlier
    p_re, p_im, q_re, q_im, s_re, s_im = later
    return (
        p_re * a_re - p_im * a_im,
        p_re * a_im + p_im * a_re,
        p_re * b_re - p_im * b_im + q_re,
        p_re * b_im + p_im * b_re + q_im,
        p_re * c_re + p_im * c_im + s_re,
        p_re * c_im - p_im * c_re + s_im,
    )


def apply_carry(local, carry):
    prod_re, prod_im, state_re, state_im, adjoint_re, adjoint_im = local
    enter_re = carry[2][None, :]
    enter_im = carry[3][None, :]
    back_enter_re = carry[4][None, :]
    back_enter_im = carry[5][None, :]
    state_re = state_re + prod_re * enter_re - prod_im * enter_im
    state_im = state_im + prod_re * enter_im + prod_im * enter_re
    adjoint_re = adjoint_re + prod_re * back_enter_re + prod_im * back_enter_im
    adjoint_im = adjoint_im + prod_re * back_enter_im - prod_im * back_enter_re
    return (state_re, state_im, adjoint_re, adjoint_im)


def rms_normed(block_in, norm_gain):
    widened = block_in.astype(F32)
    spread = jnp.mean(widened * widened, axis=1, keepdims=True)
    return widened, (widened * lax.rsqrt(spread + epsilon) * norm_gain).astype(BF16)


def body_any(tokens, token_ids, norm_gain, w_in, rates, phases, forget, readout, skip, out_grad):
    block_ids = token_ids[0]
    block_grad = out_grad[0]
    pairs = rates.shape[0]
    widened, normed = rms_normed(tokens[0], norm_gain)
    inputs = jnp.dot(
        normed, lax.all_gather(w_in, "fsdp", axis=0, tiled=True), preferred_element_type=F32
    )
    radius = jnp.exp(-rates)
    in_scale = jnp.sqrt(-jnp.expm1(-2.0 * rates))
    up_re = readout[0]
    up_im = readout[1]
    retain = jnp.where(block_ids[:, None] >= first_special, 1.0 - forget[None, :], 1.0)
    decay_re = retain * radius * jnp.cos(phases)
    decay_im = retain * radius * jnp.sin(phases)
    drive_re = in_scale * inputs[:, :pairs]
    drive_im = in_scale * inputs[:, pairs:]
    grad_wide = block_grad.astype(F32)
    state_re = up_re * grad_wide[:, :pairs] + up_im * grad_wide[:, pairs:]
    state_im = up_re * grad_wide[:, pairs:] - up_im * grad_wide[:, :pairs]
    back_re = decay_re * state_re + decay_im * state_im
    back_im = decay_re * state_im - decay_im * state_re
    elements = (decay_re, decay_im, drive_re, drive_im, back_re, back_im)
    ahead = lax.associative_scan(chain_join, elements, axis=0)
    behind = lax.associative_scan(chain_join, elements, reverse=True, axis=0)
    ahead_summary = tuple((member[-1] for member in ahead))
    behind_summary = tuple((member[0] for member in behind))
    ones_row = jnp.ones((pairs,), F32)
    zeros_row = jnp.zeros((pairs,), F32)
    identity = (ones_row, zeros_row, zeros_row, zeros_row, zeros_row, zeros_row)
    ahead_in = carried_in(ahead_summary, "seq", chain_join, identity, False)
    behind_in = carried_in(behind_summary, "seq", chain_join, identity, True)
    fwd_re, fwd_im, sigma_re, sigma_im = apply_carry(ahead, ahead_in)
    bwd_re, bwd_im, rho_re, rho_im = apply_carry(behind, behind_in)
    sum_re = fwd_re + bwd_re
    sum_im = fwd_im + bwd_im
    out_re = up_re * sum_re - up_im * sum_im
    out_im = up_re * sum_im + up_im * sum_re
    branch = jnp.concatenate([out_re, out_im], axis=1)
    mixed = (widened + branch + skip * normed.astype(F32)).astype(BF16)
    later_re = jnp.concatenate([rho_re[1:], behind_in[4][None, :]], axis=0)
    later_im = jnp.concatenate([rho_im[1:], behind_in[5][None, :]], axis=0)
    former_re = jnp.concatenate([ahead_in[4][None, :], sigma_re[:-1]], axis=0)
    former_im = jnp.concatenate([ahead_in[5][None, :], sigma_im[:-1]], axis=0)
    grad_re = in_scale * (2.0 * state_re + later_re + former_re)
    grad_im = in_scale * (2.0 * state_im + later_im + former_im)
    input_grad = jnp.concatenate([grad_re, grad_im], axis=1).astype(BF16)
    row_block = lax.psum_scatter(
        lax.dot_general(
            normed, input_grad, (((0,), (0,)), ((), ())), preferred_element_type=F32
        ),
        "fsdp",
        scatter_dimension=0,
        tiled=True,
    )
    grad_w_in = lax.psum_scatter(row_block, "seq", scatter_dimension=1, tiled=True)
    return (mixed[None], grad_w_in)


SLAB = ("x", "y", "c")
PIECES = 4
PLACES = [(k % 2, k // 2 % 2, k // 4) for k in range(8)]


def flip(value, *axes):
    count = 2 ** len(axes)
    return lax.ppermute(value, axes, [(i, count - 1 - i) for i in range(count)])


def z_flip(value, distance, count):
    return lax.ppermute(value, "z", [(i, i ^ distance) for i in range(count)])


def exchange(value, axes):
    return lax.all_to_all(value, axes, 0, 0, tiled=True)


def cmul(a_re, a_im, b_re, b_im):
    return a_re * b_re - a_im * b_im, a_re * b_im + a_im * b_re


def iota(shape, dim):
    return lax.broadcasted_iota(jnp.int32, shape, dim)


def reorder(half, back=False):
    steps = half // ROWS
    row, position = iota((half, half), int(back)), iota((half, half), 1 - int(back))
    hit = position == lax.rem(row, ROWS) * steps + lax.div(row, ROWS)
    return jnp.where(hit, 1.0, 0.0).astype(BF16)


def cut_kernel(w, *outs):
    wide = outs[0].shape[1] // 2
    for d, out in enumerate(outs):
        dy, dc = divmod(d, 2)
        here = positions()
        to = (here["x"] * 2 + (here["y"] ^ dy)) * 2 + (here["c"] ^ dc)
        for part in range(2):
            columns = pl.ds(pl.multiple_of(to * wide + part * (w.shape[1] // 2), wide), wide)
            out[:, part * wide : (part + 1) * wide] = w[:, columns]


def stack_kernel(*refs):
    pieces, out = refs[:-1], refs[-1]
    here = positions()
    for d, piece in enumerate(pieces):
        dy, dc = divmod(d, 2)
        out[(here["y"] ^ dy) * 2 + (here["c"] ^ dc)] = piece[...]


def rms_rows(tokens, gain):
    widened = tokens.astype(F32)
    spread = jnp.mean(widened * widened, axis=1, keepdims=True)
    return widened, (widened * lax.rsqrt(spread + epsilon) * gain).astype(BF16)


def norm_kernel(tokens, gain, far, near, held):
    _, normed = rms_rows(tokens[0], gain[...])
    held[...] = jnp.dot(reorder(held.shape[0]), normed, preferred_element_type=F32).astype(BF16)
    side = lax.div(positions()["z"], 2)
    for out, index in ((far, 1 - side), (near, side)):
        width = out.shape[1]
        out[...] = held[:, pl.ds(pl.multiple_of(index * width, width), width)]


def grad_kernel(grad, ids, out):
    members, rows, both = out.shape
    half, wide = grad.shape[1], both // 2
    steps = half // ROWS
    moved = jnp.dot(reorder(half), grad[0], preferred_element_type=F32).astype(BF16)
    special = jnp.where(ids[...] >= first_special, 1.0, 0.0).astype(F32)
    under = (rows - half, half)
    spread = jnp.where(lax.div(iota(under, 1), steps) == iota(under, 0), special, 0.0).astype(BF16)
    pick = jnp.where(lax.rem(iota((half, both), 0), steps) == iota((half, both), 1), 1.0, 0.0)
    flags = jnp.dot(spread, pick.astype(BF16), preferred_element_type=F32).astype(BF16)
    for m in range(members):
        for part in range(2):
            at = (part * members + m) * wide
            out[m, :half, part * wide : (part + 1) * wide] = moved[:, at : at + wide]
        out[m, half:, :] = flags


def scan_chunks(x_re, x_im, p_re, p_im, backward):
    rows = iota(x_re.shape, 0)

    def moved(value, by, fill):
        if backward:
            return jnp.where(rows < ROWS - by, pltpu.roll(value, ROWS - by, 0), fill)
        return jnp.where(rows >= by, pltpu.roll(value, by, 0), fill)

    by = 1
    while by < ROWS:
        add_re, add_im = cmul(p_re, p_im, moved(x_re, by, 0.0), moved(x_im, by, 0.0))
        p_re, p_im = cmul(p_re, p_im, moved(p_re, by, 1.0), moved(p_im, by, 0.0))
        x_re, x_im = x_re + add_re, x_im + add_im
        by *= 2
    end = 0 if backward else ROWS - 1
    total = (x_re[end : end + 1, :], x_im[end : end + 1, :])
    enter = (moved(x_re, 1, 0.0), moved(x_im, 1, 0.0))
    decay = (moved(p_re, 1, 1.0), moved(p_im, 1, 0.0))
    return total, enter, decay


def both_ways(adjoint, group, pars, keep, val, res):
    blocks, steps, _, wide = keep.shape
    count = blocks // 2
    lam_re = jnp.broadcast_to(pars[0:1, :], (ROWS, wide))
    lam_im = jnp.broadcast_to(pars[1:2, :], (ROWS, wide))
    if adjoint:
        lam_im = -lam_im
    pow_re, pow_im = lam_re, lam_im
    done = 1
    while done < steps:
        pow_re, pow_im = cmul(pow_re, pow_im, pow_re, pow_im)
        done *= 2
    zero = jnp.zeros((ROWS, wide), F32)

    def step(m, j, state):
        held, v_re, v_im = keep[m, j], val[0, m, j], val[1, m, j]
        if adjoint:
            out = (v_re + state[0], v_im + state[1])
            n_re, n_im = cmul(lam_re, lam_im, *out)
            return (held * n_re, held * n_im), out
        n_re, n_im = cmul(lam_re, lam_im, held * state[0], held * state[1])
        n_re, n_im = n_re + v_re, n_im + v_im
        return (n_re, n_im), (n_re, n_im)

    for first in range(0, count, group):
        chains = [x * count + q for q in range(first, first + group) for x in range(2)]
        ahead = {m: (zero, zero) for m in chains}
        behind = {m: (zero, zero) for m in chains}
        kept = {m: zero + 1.0 for m in chains}
        for i in range(steps):
            for m in chains:
                ahead[m], _ = step(m, i, ahead[m])
                behind[m], _ = step(m, steps - 1 - i, behind[m])
                kept[m] = kept[m] * keep[m, i]
        for q in range(first, first + group):
            for states, order, backward in ((ahead, (q, count + q), False), (behind, (count + q, q), True)):
                near, far = order
                total, enter, _ = scan_chunks(
                    *states[near], kept[near] * pow_re, kept[near] * pow_im, backward
                )
                _, later, decay = scan_chunks(
                    *states[far], kept[far] * pow_re, kept[far] * pow_im, backward
                )
                add_re, add_im = cmul(*decay, *total)
                states[near] = enter
                states[far] = (later[0] + add_re, later[1] + add_im)
        for i in range(steps):
            for m in chains:
                ahead[m], out_a = step(m, i, ahead[m])
                behind[m], out_b = step(m, steps - 1 - i, behind[m])
                for part in range(2):
                    if i < steps // 2:
                        res[part, m, i] = out_a[part]
                        res[part, m, steps - 1 - i] = out_b[part]
                    else:
                        res[part, m, i] = res[part, m, i] + out_a[part]
                        res[part, m, steps - 1 - i] = res[part, m, steps - 1 - i] + out_b[part]


def fill_keep(m, chunk, pars, keep):
    steps = keep.shape[1]
    lose = jnp.broadcast_to(pars[2:3, :], keep.shape[-2:])
    for j in range(steps):
        keep[m, j] = 1.0 - jnp.broadcast_to(chunk[:, j : j + 1], lose.shape) * lose


def adjoint_kernel(og, pars, ig, flags, keep, val, res):
    blocks, steps, _, wide = keep.shape
    half = steps * ROWS
    shape = (steps, ROWS, wide)
    c_re, c_im = pars[3:4, :], pars[4:5, :]
    for m in range(blocks):
        chunk = og[m, half:, :].astype(F32)[:ROWS, :wide]
        flags[m] = chunk
        fill_keep(m, chunk, pars, keep)
        q_re = og[m, :half, :wide].astype(F32)
        q_im = og[m, :half, wide:].astype(F32)
        val[0, m] = (c_re * q_re + c_im * q_im).reshape(shape)
        val[1, m] = (c_re * q_im - c_im * q_re).reshape(shape)
    both_ways(True, 2, pars, keep, val, res)
    for m in range(blocks):
        for part in range(2):
            block = res[part, m].reshape(half, wide)
            ig[part * wide : (part + 1) * wide, m * half : (m + 1) * half] = block.T.astype(BF16)


def pack(pieces, here, out, columns=None):
    for (dx, dy, dc), piece in pieces:
        m = ((here["x"] ^ dx) * 2 + (here["y"] ^ dy)) * 2 + (here["c"] ^ dc)
        if columns is None:
            out[m] = piece[...]
        else:
            out[m, :, columns] = piece[...]


def positions():
    return {axis: lax.axis_index(axis) for axis in ("x", "z", "y", "c")}


def split_refs(refs, count):
    return list(zip(PLACES, refs[:count])), refs[count:]


def forward_kernel(n_z, *refs):
    near, refs = split_refs(refs, len(PLACES))
    far, refs = split_refs(refs, len(PLACES))
    wbs, refs = refs[:n_z], refs[n_z:]
    flags, pars, branch, n_all, w_all, keep, val, res = refs
    blocks, steps, _, wide = keep.shape
    half = steps * ROWS
    here = positions()
    for dz in range(n_z):
        w_all[dz // 2 * 2 + lax.rem(here["z"] ^ dz, 2)] = wbs[dz][...].reshape(w_all.shape[1:])
    middle = n_all.shape[2] // 2
    pack(near, here, n_all, slice(0, middle))
    pack(far, here, n_all, slice(middle, 2 * middle))
    for m in range(blocks):
        fill_keep(m, flags[m], pars, keep)
    model = n_all.shape[2]
    got = jnp.dot(
        n_all[...].reshape(blocks * half, model),
        w_all[...].reshape(model, 2 * wide),
        preferred_element_type=F32,
    )
    val[0] = got[:, :wide].reshape(blocks, steps, ROWS, wide)
    val[1] = got[:, wide:].reshape(blocks, steps, ROWS, wide)
    both_ways(False, 2, pars, keep, val, res)
    c_re, c_im = pars[3:4, :], pars[4:5, :]
    for m in range(blocks):
        s_re = res[0, m].reshape(half, wide)
        s_im = res[1, m].reshape(half, wide)
        branch[m, :, :wide] = (c_re * s_re - c_im * s_im).astype(BF16)
        branch[m, :, wide:] = (c_re * s_im + c_im * s_re).astype(BF16)


def outer_kernel(across, *refs):
    pieces, refs = split_refs(refs, len(PLACES))
    ig, outs, n_cut = refs[0], refs[1:-1], refs[-1]
    here = positions()
    blocks, half, _ = n_cut.shape
    pack(pieces, here, n_cut)
    for k, out in enumerate(outs):
        at = lax.rem(here["z"] + 1 - k, 2) * across
        columns = pl.ds(pl.multiple_of(at, across), across)
        rows = n_cut[:, :, columns].reshape(blocks * half, across)
        out[...] = jnp.dot(ig[...], rows, preferred_element_type=F32).astype(out.dtype)


def sum_kernel(*refs):
    count = (len(refs) - 2) // 2
    sent, out, held, done = refs[:count], refs[count], refs[count + 1 : -1], refs[-1]
    copies = [pltpu.make_async_copy(src, dst, done.at[k]) for k, (src, dst) in enumerate(zip(sent, held))]
    for copy in copies:
        copy.start()
    for copy in copies:
        copy.wait()
    members, rows, wide = out.shape
    total = held[0][...]
    for other in held[1:]:
        total = total + other[...].astype(F32)
    across = members // 2
    for part in range(2):
        for d in range(across):
            block = total[part * wide : (part + 1) * wide, d * rows : (d + 1) * rows]
            out[part * across + d] = block.T.astype(BF16)


def place_kernel(got, out):
    members, _, wide = got.shape
    for m in range(members):
        out[:, m * wide : (m + 1) * wide] = got[m].astype(F32)


def mixed_kernel(tokens, gain, skip, branch, out):
    members, half, both = branch.shape
    wide = both // 2
    widened, normed = rms_rows(tokens[0], gain[...])
    base = widened + skip[...] * normed.astype(F32)
    back = reorder(half, True)
    for m in range(members):
        got = jnp.dot(back, branch[m], preferred_element_type=F32)
        for part in range(2):
            columns = slice((part * members + m) * wide, (part * members + m + 1) * wide)
            total = base[:, columns] + got[:, part * wide : (part + 1) * wide]
            out[0, :, columns] = total.astype(BF16)


def call(kernel, out_shape, inputs, scratch=(), mib=8, flops=1_000_000, space=pltpu.VMEM):
    vmem = pl.BlockSpec(memory_space=pltpu.VMEM)
    made = jax.tree.leaves(out_shape)
    moved = sum(a.size * a.dtype.itemsize for a in [*inputs, *made])
    return pl.pallas_call(
        kernel,
        out_shape=out_shape,
        in_specs=[pl.BlockSpec(memory_space=space)] * len(inputs),
        out_specs=jax.tree.map(lambda _: vmem, out_shape),
        scratch_shapes=list(scratch),
        compiler_params=pltpu.CompilerParams(vmem_limit_bytes=mib * 2**20),
        cost_estimate=pl.CostEstimate(flops=flops, bytes_accessed=moved, transcendentals=0),
    )(*inputs)


def body_slab(layout, *inputs):
    return slab_step(layout, *inputs)


def slab_step(layout, tokens, token_ids, norm_gain, w_in, rates, phases, forget, readout, skip, out_grad):
    half, model = tokens.shape[1:]
    pairs = rates.shape[0]
    n_z, count = layout["z"], PIECES
    members = 2 * count
    wide = pairs // members
    steps = half // ROWS
    mine = (lax.axis_index("x") * 2 + lax.axis_index("y")) * 2 + lax.axis_index("c")

    def shaped(shape, dtype=BF16):
        return jax.ShapeDtypeStruct(shape, dtype)

    w_cut = call(cut_kernel, [shaped((w_in.shape[0], 2 * wide))] * count, [w_in])
    w_cut = list(w_cut)
    w_cut[1] = flip(w_cut[1], "c")
    w_cut[2] = flip(w_cut[2], "y")
    w_cut[3] = flip(w_cut[3], "y", "c")
    w_own = call(stack_kernel, shaped((count, w_in.shape[0], 2 * wide)), w_cut)
    w_2 = z_flip(w_own, 2, n_z)
    w_1 = z_flip(w_own, 1, n_z)
    w_3 = z_flip(w_2, 1, n_z)

    gain = norm_gain.reshape(1, model)
    far, near = call(
        norm_kernel, [shaped((half, model // 2))] * 2, [tokens, gain], [pltpu.VMEM((half, model), BF16)]
    )
    far_x, far_y = flip(far, "x"), flip(far, "y")
    far_xy = flip(far_y, "x")
    near_x, near_y = flip(near, "x"), flip(near, "y")
    near_xy = flip(near_x, "y")
    far = [far, far_x, far_y, far_xy]
    near = [near, near_x, near_y, near_xy]
    far += [flip(piece, "c") for piece in far]
    near += [flip(piece, "c") for piece in near]

    under = 16
    og = call(grad_kernel, shaped((members, half + under, 2 * wide)), [out_grad, token_ids])
    og = exchange(og, SLAB)

    radius = jnp.exp(-rates)
    in_scale = jnp.sqrt(-jnp.expm1(-2.0 * rates))
    rows = [radius * jnp.cos(phases), radius * jnp.sin(phases), forget, in_scale * readout[0], in_scale * readout[1]]
    rows = jnp.stack(rows + [jnp.zeros_like(rates)] * (ROWS - len(rows)))
    pars = lax.dynamic_slice_in_dim(rows, mine * wide, wide, axis=1)

    chains = [
        pltpu.VMEM((members, steps, ROWS, wide), F32),
        pltpu.VMEM((2, members, steps, ROWS, wide), F32),
        pltpu.VMEM((2, members, steps, ROWS, wide), F32),
    ]
    ig, flags = call(
        adjoint_kernel,
        [shaped((2 * wide, members * half)), shaped((members, ROWS, wide), F32)],
        [og, pars],
        chains,
        flops=20_000_000,
    )

    across = model // n_z
    matmul = 2 * members * half * model * 2 * wide
    parts = []
    for pieces, kind in ((far, BF16), (near, F32)):
        parts += call(
            functools.partial(outer_kernel, across),
            [shaped((2 * wide, across)), shaped((2 * wide, across), kind)],
            [*pieces, ig],
            [pltpu.VMEM((members, half, model // 2), BF16)],
            mib=16,
            flops=matmul // 2,
        )
    got = [z_flip(part, dz, n_z) for dz, part in zip((3, 2, 1), parts)]

    branch = call(
        functools.partial(forward_kernel, n_z),
        shaped((members, half, 2 * wide)),
        [*near, *far, w_own, w_1, w_2, w_3, flags, pars],
        [pltpu.VMEM((members, half, model), BF16), pltpu.VMEM((n_z, model // n_z, 2 * wide), BF16)] + chains,
        mib=24,
        flops=matmul,
    )
    branch = exchange(branch, SLAB)
    mixed = call(
        mixed_kernel, shaped(tokens.shape), [tokens, gain, skip.reshape(1, model), branch], flops=10_000_000
    )

    sums = [parts[3], *got]
    total = call(
        sum_kernel,
        shaped((members, across // count, wide)),
        sums,
        [*(pltpu.VMEM(part.shape, part.dtype) for part in sums), pltpu.SemaphoreType.DMA((len(sums),))],
        space=pl.ANY,
    )
    total = exchange(total, SLAB)
    grad_w_in = call(place_kernel, shaped((across // count, pairs), F32), [total])
    return (mixed, grad_w_in)


def solution(mesh):
    n_seq, n_fsdp = mesh.shape["seq"], mesh.shape["fsdp"]
    if n_seq == 2 and n_fsdp == 16:
        layout = {"x": n_seq, "z": n_fsdp // 4, "y": 2, "c": 2}
        mesh = Mesh(mesh.devices.reshape(tuple(layout.values())), tuple(layout))
        body, fsdp, seq = functools.partial(body_slab, layout), ("z", "y", "c"), "x"
    else:
        body, fsdp, seq = body_any, "fsdp", "seq"
    in_specs = (
        P(fsdp, seq, None),
        P(fsdp, seq),
        P(),
        P(fsdp, None),
        P(),
        P(),
        P(),
        P(),
        P(),
        P(fsdp, seq, None),
    )
    out_specs = (P(fsdp, seq, None), P(fsdp, seq))
    return jax.shard_map(body, mesh=mesh, in_specs=in_specs, out_specs=out_specs, check_vma=False)
```

```python
import functools

import jax
import jax.numpy as jnp
from jax import lax
from jax.experimental import pallas as pl
from jax.experimental.pallas import tpu as pltpu
from jax.sharding import Mesh, PartitionSpec as P


epsilon = 1e-06
first_special = 4
ROWS = 8
BF16 = jnp.bfloat16
F32 = jnp.float32


def carried_in(value, axis, join, neutral, backward):
    count, mine = (lax.axis_size(axis), lax.axis_index(axis))
    pieces = jax.tree.map(lambda part: lax.all_gather(part, axis), value)
    if backward:
        pieces = jax.tree.map(lambda part: part[::-1], pieces)
        mine = count - 1 - mine
    running = jax.tree.map(
        lambda part, zero: jnp.full_like(part, 0) + jnp.asarray(zero, part.dtype), value, neutral
    )

    def turn(position, running):
        longer = join(running, jax.tree.map(lambda part: part[position], pieces))
        return jax.tree.map(lambda new, old: jnp.where(position < mine, new, old), longer, running)

    return lax.fori_loop(0, count - 1, turn, running)


def chain_join(earlier, later):
    a_re, a_im, b_re, b_im, c_re, c_im = earlier
    p_re, p_im, q_re, q_im, s_re, s_im = later
    return (
        p_re * a_re - p_im * a_im,
        p_re * a_im + p_im * a_re,
        p_re * b_re - p_im * b_im + q_re,
        p_re * b_im + p_im * b_re + q_im,
        p_re * c_re + p_im * c_im + s_re,
        p_re * c_im - p_im * c_re + s_im,
    )


def apply_carry(local, carry):
    prod_re, prod_im, state_re, state_im, adjoint_re, adjoint_im = local
    enter_re = carry[2][None, :]
    enter_im = carry[3][None, :]
    back_enter_re = carry[4][None, :]
    back_enter_im = carry[5][None, :]
    state_re = state_re + prod_re * enter_re - prod_im * enter_im
    state_im = state_im + prod_re * enter_im + prod_im * enter_re
    adjoint_re = adjoint_re + prod_re * back_enter_re + prod_im * back_enter_im
    adjoint_im = adjoint_im + prod_re * back_enter_im - prod_im * back_enter_re
    return (state_re, state_im, adjoint_re, adjoint_im)


def rms_normed(block_in, norm_gain):
    widened = block_in.astype(F32)
    spread = jnp.mean(widened * widened, axis=1, keepdims=True)
    return widened, (widened * lax.rsqrt(spread + epsilon) * norm_gain).astype(BF16)


def body_any(tokens, token_ids, norm_gain, w_in, rates, phases, forget, readout, skip, out_grad):
    block_ids = token_ids[0]
    block_grad = out_grad[0]
    pairs = rates.shape[0]
    widened, normed = rms_normed(tokens[0], norm_gain)
    inputs = jnp.dot(
        normed, lax.all_gather(w_in, "fsdp", axis=0, tiled=True), preferred_element_type=F32
    )
    radius = jnp.exp(-rates)
    in_scale = jnp.sqrt(-jnp.expm1(-2.0 * rates))
    up_re = readout[0]
    up_im = readout[1]
    retain = jnp.where(block_ids[:, None] >= first_special, 1.0 - forget[None, :], 1.0)
    decay_re = retain * radius * jnp.cos(phases)
    decay_im = retain * radius * jnp.sin(phases)
    drive_re = in_scale * inputs[:, :pairs]
    drive_im = in_scale * inputs[:, pairs:]
    grad_wide = block_grad.astype(F32)
    state_re = up_re * grad_wide[:, :pairs] + up_im * grad_wide[:, pairs:]
    state_im = up_re * grad_wide[:, pairs:] - up_im * grad_wide[:, :pairs]
    back_re = decay_re * state_re + decay_im * state_im
    back_im = decay_re * state_im - decay_im * state_re
    elements = (decay_re, decay_im, drive_re, drive_im, back_re, back_im)
    ahead = lax.associative_scan(chain_join, elements, axis=0)
    behind = lax.associative_scan(chain_join, elements, reverse=True, axis=0)
    ahead_summary = tuple((member[-1] for member in ahead))
    behind_summary = tuple((member[0] for member in behind))
    ones_row = jnp.ones((pairs,), F32)
    zeros_row = jnp.zeros((pairs,), F32)
    identity = (ones_row, zeros_row, zeros_row, zeros_row, zeros_row, zeros_row)
    ahead_in = carried_in(ahead_summary, "seq", chain_join, identity, False)
    behind_in = carried_in(behind_summary, "seq", chain_join, identity, True)
    fwd_re, fwd_im, sigma_re, sigma_im = apply_carry(ahead, ahead_in)
    bwd_re, bwd_im, rho_re, rho_im = apply_carry(behind, behind_in)
    sum_re = fwd_re + bwd_re
    sum_im = fwd_im + bwd_im
    out_re = up_re * sum_re - up_im * sum_im
    out_im = up_re * sum_im + up_im * sum_re
    branch = jnp.concatenate([out_re, out_im], axis=1)
    mixed = (widened + branch + skip * normed.astype(F32)).astype(BF16)
    later_re = jnp.concatenate([rho_re[1:], behind_in[4][None, :]], axis=0)
    later_im = jnp.concatenate([rho_im[1:], behind_in[5][None, :]], axis=0)
    former_re = jnp.concatenate([ahead_in[4][None, :], sigma_re[:-1]], axis=0)
    former_im = jnp.concatenate([ahead_in[5][None, :], sigma_im[:-1]], axis=0)
    grad_re = in_scale * (2.0 * state_re + later_re + former_re)
    grad_im = in_scale * (2.0 * state_im + later_im + former_im)
    input_grad = jnp.concatenate([grad_re, grad_im], axis=1).astype(BF16)
    row_block = lax.psum_scatter(
        lax.dot_general(
            normed, input_grad, (((0,), (0,)), ((), ())), preferred_element_type=F32
        ),
        "fsdp",
        scatter_dimension=0,
        tiled=True,
    )
    grad_w_in = lax.psum_scatter(row_block, "seq", scatter_dimension=1, tiled=True)
    return (mixed[None], grad_w_in)


SLAB = ("x", "y", "c")
PIECES = 4
FIRST, SECOND = (3, 2), (1, 0)
PLACES = [(k % 2, k // 2 % 2, k // 4) for k in range(8)]
CUT_PLACES = [place for place in PLACES for _ in range(1 + place[0] * place[1])]


def flip(value, *axes):
    count = 2 ** len(axes)
    return lax.ppermute(value, axes, [(i, count - 1 - i) for i in range(count)])


def z_flip(value, distance, count):
    return lax.ppermute(value, "z", [(i, i ^ distance) for i in range(count)])


def exchange(value, axes):
    return lax.all_to_all(value, axes, 0, 0, tiled=True)


def cmul(a_re, a_im, b_re, b_im):
    return a_re * b_re - a_im * b_im, a_re * b_im + a_im * b_re


def iota(shape, dim):
    return lax.broadcasted_iota(jnp.int32, shape, dim)


def reorder(half, back=False):
    steps = half // ROWS
    row, position = iota((half, half), int(back)), iota((half, half), 1 - int(back))
    hit = position == lax.rem(row, ROWS) * steps + lax.div(row, ROWS)
    return jnp.where(hit, 1.0, 0.0).astype(BF16)


def cut_kernel(w, *outs):
    wide = outs[0].shape[1] // 2
    for d, out in enumerate(outs):
        dy, dc = divmod(d, 2)
        here = positions()
        to = (here["x"] * 2 + (here["y"] ^ dy)) * 2 + (here["c"] ^ dc)
        for part in range(2):
            columns = pl.ds(pl.multiple_of(to * wide + part * (w.shape[1] // 2), wide), wide)
            out[:, part * wide : (part + 1) * wide] = w[:, columns]


def stack_kernel(*refs):
    pieces, out = refs[:-1], refs[-1]
    here = positions()
    for d, piece in enumerate(pieces):
        dy, dc = divmod(d, 2)
        out[(here["y"] ^ dy) * 2 + (here["c"] ^ dc)] = piece[...]


def rms_rows(tokens, gain):
    widened = tokens.astype(F32)
    spread = jnp.mean(widened * widened, axis=1, keepdims=True)
    return widened, (widened * lax.rsqrt(spread + epsilon) * gain).astype(BF16)


def norm_kernel(tokens, gain, first, second, rows, held, done):
    copy = pltpu.make_async_copy(tokens, rows, done)
    copy.start()
    copy.wait()
    _, normed = rms_rows(rows[0], gain[...])
    held[...] = jnp.dot(reorder(held.shape[0]), normed, preferred_element_type=F32).astype(BF16)
    width = first.shape[1] // 2
    for out, distances in ((first, FIRST), (second, SECOND)):
        for k, dz in enumerate(distances):
            at = pl.multiple_of((positions()["z"] ^ dz) * width, width)
            out[:, k * width : (k + 1) * width] = held[:, pl.ds(at, width)]


def grad_kernel(grad, ids, out):
    members, rows, both = out.shape
    half, wide = grad.shape[1], both // 2
    steps = half // ROWS
    moved = jnp.dot(reorder(half), grad[0], preferred_element_type=F32).astype(BF16)
    special = jnp.where(ids[...] >= first_special, 1.0, 0.0).astype(F32)
    under = (rows - half, half)
    spread = jnp.where(lax.div(iota(under, 1), steps) == iota(under, 0), special, 0.0).astype(BF16)
    pick = jnp.where(lax.rem(iota((half, both), 0), steps) == iota((half, both), 1), 1.0, 0.0)
    flags = jnp.dot(spread, pick.astype(BF16), preferred_element_type=F32).astype(BF16)
    for m in range(members):
        for part in range(2):
            at = (part * members + m) * wide
            out[m, :half, part * wide : (part + 1) * wide] = moved[:, at : at + wide]
        out[m, half:, :] = flags


def scan_chunks(x_re, x_im, p_re, p_im, backward):
    rows = iota(x_re.shape, 0)

    def moved(value, by, fill):
        if backward:
            return jnp.where(rows < ROWS - by, pltpu.roll(value, ROWS - by, 0), fill)
        return jnp.where(rows >= by, pltpu.roll(value, by, 0), fill)

    by = 1
    while by < ROWS:
        add_re, add_im = cmul(p_re, p_im, moved(x_re, by, 0.0), moved(x_im, by, 0.0))
        p_re, p_im = cmul(p_re, p_im, moved(p_re, by, 1.0), moved(p_im, by, 0.0))
        x_re, x_im = x_re + add_re, x_im + add_im
        by *= 2
    end = 0 if backward else ROWS - 1
    total = (x_re[end : end + 1, :], x_im[end : end + 1, :])
    enter = (moved(x_re, 1, 0.0), moved(x_im, 1, 0.0))
    decay = (moved(p_re, 1, 1.0), moved(p_im, 1, 0.0))
    return total, enter, decay


def both_ways(adjoint, group, pars, keep, val, res):
    blocks, steps, _, wide = keep.shape
    count = blocks // 2
    lam_re = jnp.broadcast_to(pars[0:1, :], (ROWS, wide))
    lam_im = jnp.broadcast_to(pars[1:2, :], (ROWS, wide))
    if adjoint:
        lam_im = -lam_im
    pow_re, pow_im = lam_re, lam_im
    done = 1
    while done < steps:
        pow_re, pow_im = cmul(pow_re, pow_im, pow_re, pow_im)
        done *= 2
    zero = jnp.zeros((ROWS, wide), F32)

    def step(m, j, state):
        held, v_re, v_im = keep[m, j], val[0, m, j], val[1, m, j]
        if adjoint:
            out = (v_re + state[0], v_im + state[1])
            n_re, n_im = cmul(lam_re, lam_im, *out)
            return (held * n_re, held * n_im), out
        n_re, n_im = cmul(lam_re, lam_im, held * state[0], held * state[1])
        n_re, n_im = n_re + v_re, n_im + v_im
        return (n_re, n_im), (n_re, n_im)

    for first in range(0, count, group):
        chains = [x * count + q for q in range(first, first + group) for x in range(2)]
        ahead = {m: (zero, zero) for m in chains}
        behind = {m: (zero, zero) for m in chains}
        kept = {m: zero + 1.0 for m in chains}
        for i in range(steps):
            for m in chains:
                ahead[m], _ = step(m, i, ahead[m])
                behind[m], _ = step(m, steps - 1 - i, behind[m])
                kept[m] = kept[m] * keep[m, i]
        for q in range(first, first + group):
            for states, order, backward in ((ahead, (q, count + q), False), (behind, (count + q, q), True)):
                near, far = order
                total, enter, _ = scan_chunks(
                    *states[near], kept[near] * pow_re, kept[near] * pow_im, backward
                )
                _, later, decay = scan_chunks(
                    *states[far], kept[far] * pow_re, kept[far] * pow_im, backward
                )
                add_re, add_im = cmul(*decay, *total)
                states[near] = enter
                states[far] = (later[0] + add_re, later[1] + add_im)
        for i in range(steps):
            for m in chains:
                ahead[m], out_a = step(m, i, ahead[m])
                behind[m], out_b = step(m, steps - 1 - i, behind[m])
                for part in range(2):
                    if i < steps // 2:
                        res[part, m, i] = out_a[part]
                        res[part, m, steps - 1 - i] = out_b[part]
                    else:
                        res[part, m, i] = res[part, m, i] + out_a[part]
                        res[part, m, steps - 1 - i] = res[part, m, steps - 1 - i] + out_b[part]


def fill_keep(m, chunk, pars, keep):
    steps = keep.shape[1]
    lose = jnp.broadcast_to(pars[2:3, :], keep.shape[-2:])
    for j in range(steps):
        keep[m, j] = 1.0 - jnp.broadcast_to(chunk[:, j : j + 1], lose.shape) * lose


def adjoint_kernel(og, pars, ig, flags, keep, val, res):
    blocks, steps, _, wide = keep.shape
    half = steps * ROWS
    shape = (steps, ROWS, wide)
    c_re, c_im = pars[3:4, :], pars[4:5, :]
    for m in range(blocks):
        chunk = og[m, half:, :].astype(F32)[:ROWS, :wide]
        flags[m] = chunk
        fill_keep(m, chunk, pars, keep)
        q_re = og[m, :half, :wide].astype(F32)
        q_im = og[m, :half, wide:].astype(F32)
        val[0, m] = (c_re * q_re + c_im * q_im).reshape(shape)
        val[1, m] = (c_re * q_im - c_im * q_re).reshape(shape)
    both_ways(True, 2, pars, keep, val, res)
    for m in range(blocks):
        for part in range(2):
            block = res[part, m].reshape(half, wide)
            ig[part * wide : (part + 1) * wide, m * half : (m + 1) * half] = block.T.astype(BF16)


def pack(pieces, here, out, columns=slice(None)):
    half = out.shape[1]
    starts = {}
    for piece, (dx, dy, dc) in zip(pieces, PLACES if len(pieces) == len(PLACES) else CUT_PLACES):
        m = ((here["x"] ^ dx) * 2 + (here["y"] ^ dy)) * 2 + (here["c"] ^ dc)
        start = starts.get((dx, dy, dc), 0)
        starts[dx, dy, dc] = stop = start + piece.shape[0]
        out[m, start % half : start % half + piece.shape[0], columns] = piece[...]
        assert stop <= half


def positions():
    return {axis: lax.axis_index(axis) for axis in ("x", "z", "y", "c")}


def forward_kernel(*refs):
    first, second, refs = refs[: len(CUT_PLACES)], refs[len(CUT_PLACES) :][: len(PLACES)], refs[len(CUT_PLACES + PLACES) :]
    wbs, refs = refs[:4], refs[4:]
    flags, pars, branch, n_all, w_all, keep, val, res = refs
    blocks, steps, _, wide = keep.shape
    half = steps * ROWS
    here = positions()
    for k, dz in enumerate(FIRST + SECOND):
        w_all[k] = wbs[dz][...].reshape(w_all.shape[1:])
    middle = n_all.shape[2] // 2
    pack(first, here, n_all, slice(0, middle))
    pack(second, here, n_all, slice(middle, 2 * middle))
    for m in range(blocks):
        fill_keep(m, flags[m], pars, keep)
    model = n_all.shape[2]
    got = jnp.dot(
        n_all[...].reshape(blocks * half, model),
        w_all[...].reshape(model, 2 * wide),
        preferred_element_type=F32,
    )
    val[0] = got[:, :wide].reshape(blocks, steps, ROWS, wide)
    val[1] = got[:, wide:].reshape(blocks, steps, ROWS, wide)
    both_ways(False, 2, pars, keep, val, res)
    c_re, c_im = pars[3:4, :], pars[4:5, :]
    for m in range(blocks):
        s_re = res[0, m].reshape(half, wide)
        s_im = res[1, m].reshape(half, wide)
        branch[m, :, :wide] = (c_re * s_re - c_im * s_im).astype(BF16)
        branch[m, :, wide:] = (c_re * s_im + c_im * s_re).astype(BF16)


def outer_kernel(count, *refs):
    pieces, refs = refs[:count], refs[count:]
    ig, outs, n_cut = refs[0], refs[1:-1], refs[-1]
    blocks, half, _ = n_cut.shape
    pack(pieces, positions(), n_cut)
    across = outs[0].shape[1]
    for k, out in enumerate(outs):
        rows = n_cut[:, :, k * across : (k + 1) * across].reshape(blocks * half, across)
        out[...] = jnp.dot(ig[...], rows, preferred_element_type=F32).astype(out.dtype)


def flipped(here, place):
    x, y, c = (here[axis] ^ bit for axis, bit in zip(SLAB, place))
    return (x * 2 + y) * 2 + c, x, y * 2 + c


def pre_kernel(own, other, out):
    out[...] = own[...] + other[...].astype(F32)


def sum_kernel(count, *refs):
    sent, outs, held = refs[:count], refs[count:-count - 2], refs[-count - 2 : -2]
    total, done = refs[-2:]
    copies = [pltpu.make_async_copy(src, dst, done.at[k]) for k, (src, dst) in enumerate(zip(sent, held))]
    for copy in copies:
        copy.start()
    for copy in copies:
        copy.wait()
    rows, wide = outs[0].shape
    got = held[0][...]
    for other in held[1:]:
        got = got + other[...].astype(F32)
    total[...] = got
    here = positions()
    for out, place in zip(outs, PLACES):
        _, part, d = flipped(here, place)
        at = pl.ds(pl.multiple_of(part * wide, wide), wide)
        columns = pl.ds(pl.multiple_of(d * rows, rows), rows)
        out[...] = total[at, columns].T.astype(BF16)


def place_kernel(*refs):
    got, out = refs[:-1], refs[-1]
    here = positions()
    for block, place in zip(got, PLACES):
        wide = block.shape[1]
        m, _, _ = flipped(here, place)
        out[:, pl.ds(pl.multiple_of(m * wide, wide), wide)] = block[...].astype(F32)


def mixed_kernel(tokens, gain, skip, branch, out):
    members, half, both = branch.shape
    wide = both // 2
    widened, normed = rms_rows(tokens[0], gain[...])
    base = widened + skip[...] * normed.astype(F32)
    back = reorder(half, True)
    for m in range(members):
        got = jnp.dot(back, branch[m], preferred_element_type=F32)
        for part in range(2):
            columns = slice((part * members + m) * wide, (part * members + m + 1) * wide)
            total = base[:, columns] + got[:, part * wide : (part + 1) * wide]
            out[0, :, columns] = total.astype(BF16)


def call(kernel, out_shape, inputs, scratch=(), mib=8, flops=1_000_000, spaces=None):
    vmem = pl.BlockSpec(memory_space=pltpu.VMEM)
    made = jax.tree.leaves(out_shape)
    moved = sum(a.size * a.dtype.itemsize for a in [*inputs, *made])
    return pl.pallas_call(
        kernel,
        out_shape=out_shape,
        in_specs=[pl.BlockSpec(memory_space=space) for space in spaces or [pltpu.VMEM] * len(inputs)],
        out_specs=jax.tree.map(lambda _: vmem, out_shape),
        scratch_shapes=list(scratch),
        compiler_params=pltpu.CompilerParams(vmem_limit_bytes=mib * 2**20),
        cost_estimate=pl.CostEstimate(flops=flops, bytes_accessed=moved, transcendentals=0),
    )(*inputs)


def body_slab(layout, *inputs):
    return slab_step(layout, *inputs)


def slab_step(layout, tokens, token_ids, norm_gain, w_in, rates, phases, forget, readout, skip, out_grad):
    half, model = tokens.shape[1:]
    pairs = rates.shape[0]
    n_z, count = layout["z"], PIECES
    members = 2 * count
    wide = pairs // members
    steps = half // ROWS
    mine = (lax.axis_index("x") * 2 + lax.axis_index("y")) * 2 + lax.axis_index("c")

    def shaped(shape, dtype=BF16):
        return jax.ShapeDtypeStruct(shape, dtype)

    w_cut = call(cut_kernel, [shaped((w_in.shape[0], 2 * wide))] * count, [w_in])
    w_cut = list(w_cut)
    w_cut[1] = flip(w_cut[1], "c")
    w_cut[2] = flip(w_cut[2], "y")
    w_cut[3] = flip(w_cut[3], "y", "c")
    w_own = call(stack_kernel, shaped((count, w_in.shape[0], 2 * wide)), w_cut)
    w_2 = z_flip(w_own, 2, n_z)
    w_1 = z_flip(w_own, 1, n_z)
    w_3 = z_flip(w_2, 1, n_z)

    gain = norm_gain.reshape(1, model)
    first, second = call(
        norm_kernel,
        [shaped((half, model // 2))] * 2,
        [tokens, gain],
        [pltpu.VMEM(tokens.shape, BF16), pltpu.VMEM((half, model), BF16), pltpu.SemaphoreType.DMA],
        spaces=[pl.ANY, pltpu.VMEM],
    )
    first = [first, flip(first, "x"), flip(first, "y")]
    first += [flip(first[2][: half // 2], "x"), flip(first[1][half // 2 :], "y")]
    second = [second, flip(second, "x"), flip(second, "y")]
    second.append(flip(second[2], "x"))
    first += [flip(piece, "c") for piece in first]
    second += [flip(piece, "c") for piece in second]

    under = 16
    og = call(grad_kernel, shaped((members, half + under, 2 * wide)), [out_grad, token_ids])
    og = exchange(og, SLAB)

    radius = jnp.exp(-rates)
    in_scale = jnp.sqrt(-jnp.expm1(-2.0 * rates))
    rows = [radius * jnp.cos(phases), radius * jnp.sin(phases), forget, in_scale * readout[0], in_scale * readout[1]]
    rows = jnp.stack(rows + [jnp.zeros_like(rates)] * (ROWS - len(rows)))
    pars = lax.dynamic_slice_in_dim(rows, mine * wide, wide, axis=1)

    chains = [
        pltpu.VMEM((members, steps, ROWS, wide), F32),
        pltpu.VMEM((2, members, steps, ROWS, wide), F32),
        pltpu.VMEM((2, members, steps, ROWS, wide), F32),
    ]
    ig, flags = call(
        adjoint_kernel,
        [shaped((2 * wide, members * half)), shaped((members, ROWS, wide), F32)],
        [og, pars],
        chains,
        flops=20_000_000,
    )

    across = model // n_z
    matmul = 2 * members * half * model * 2 * wide
    parts = {}
    for pieces, distances in ((first, FIRST), (second, SECOND)):
        made = call(
            functools.partial(outer_kernel, len(pieces)),
            [shaped((2 * wide, across), BF16 if dz else F32) for dz in distances],
            [*pieces, ig],
            [pltpu.VMEM((members, half, model // 2), BF16)],
            mib=16,
            flops=matmul // 2,
        )
        parts.update(zip(distances, made))
    got = [z_flip(parts[dz], dz, n_z) for dz in (3, 2, 1)]

    branch = call(
        forward_kernel,
        shaped((members, half, 2 * wide)),
        [*first, *second, w_own, w_1, w_2, w_3, flags, pars],
        [pltpu.VMEM((members, half, model), BF16), pltpu.VMEM((n_z, model // n_z, 2 * wide), BF16)] + chains,
        mib=24,
        flops=matmul,
    )
    branch = exchange(branch, SLAB)
    mixed = call(
        mixed_kernel, shaped(tokens.shape), [tokens, gain, skip.reshape(1, model), branch], flops=10_000_000
    )

    early = call(pre_kernel, shaped((2 * wide, across), F32), [parts[0], got[0]])
    sums = [early, *got[1:]]
    total = call(
        functools.partial(sum_kernel, len(sums)),
        [shaped((across // count, wide))] * members,
        sums,
        [
            *(pltpu.VMEM(part.shape, part.dtype) for part in sums),
            pltpu.VMEM((2 * wide, across), F32),
            pltpu.SemaphoreType.DMA((len(sums),)),
        ],
        mib=8,
        spaces=[pl.ANY] * len(sums),
    )
    total = [
        flip(block, *(axis for axis, bit in zip(SLAB, place) if bit)) if any(place) else block
        for block, place in zip(total, PLACES)
    ]
    grad_w_in = call(place_kernel, shaped((across // count, pairs), F32), total)
    return (mixed, grad_w_in)


def solution(mesh):
    n_seq, n_fsdp = mesh.shape["seq"], mesh.shape["fsdp"]
    if n_seq == 2 and n_fsdp == 16:
        layout = {"x": n_seq, "z": n_fsdp // 4, "y": 2, "c": 2}
        mesh = Mesh(mesh.devices.reshape(tuple(layout.values())), tuple(layout))
        body, fsdp, seq = functools.partial(body_slab, layout), ("z", "y", "c"), "x"
    else:
        body, fsdp, seq = body_any, "fsdp", "seq"
    in_specs = (
        P(fsdp, seq, None),
        P(fsdp, seq),
        P(),
        P(fsdp, None),
        P(),
        P(),
        P(),
        P(),
        P(),
        P(fsdp, seq, None),
    )
    out_specs = (P(fsdp, seq, None), P(fsdp, seq))
    step = jax.shard_map(body, mesh=mesh, in_specs=in_specs, out_specs=out_specs, check_vma=False)
    if body is body_any:
        return step
    return step
```

```python
import functools

import jax
import jax.numpy as jnp
from jax import lax
from jax.experimental import pallas as pl
from jax.experimental.pallas import tpu as pltpu
from jax.sharding import Mesh, PartitionSpec as P


epsilon = 1e-06
first_special = 4
ROWS = 8
BF16 = jnp.bfloat16
F32 = jnp.float32


def carried_in(value, axis, join, neutral, backward):
    count, mine = (lax.axis_size(axis), lax.axis_index(axis))
    pieces = jax.tree.map(lambda part: lax.all_gather(part, axis), value)
    if backward:
        pieces = jax.tree.map(lambda part: part[::-1], pieces)
        mine = count - 1 - mine
    running = jax.tree.map(
        lambda part, zero: jnp.full_like(part, 0) + jnp.asarray(zero, part.dtype), value, neutral
    )

    def turn(position, running):
        longer = join(running, jax.tree.map(lambda part: part[position], pieces))
        return jax.tree.map(lambda new, old: jnp.where(position < mine, new, old), longer, running)

    return lax.fori_loop(0, count - 1, turn, running)


def chain_join(earlier, later):
    a_re, a_im, b_re, b_im, c_re, c_im = earlier
    p_re, p_im, q_re, q_im, s_re, s_im = later
    return (
        p_re * a_re - p_im * a_im,
        p_re * a_im + p_im * a_re,
        p_re * b_re - p_im * b_im + q_re,
        p_re * b_im + p_im * b_re + q_im,
        p_re * c_re + p_im * c_im + s_re,
        p_re * c_im - p_im * c_re + s_im,
    )


def apply_carry(local, carry):
    prod_re, prod_im, state_re, state_im, adjoint_re, adjoint_im = local
    enter_re = carry[2][None, :]
    enter_im = carry[3][None, :]
    back_enter_re = carry[4][None, :]
    back_enter_im = carry[5][None, :]
    state_re = state_re + prod_re * enter_re - prod_im * enter_im
    state_im = state_im + prod_re * enter_im + prod_im * enter_re
    adjoint_re = adjoint_re + prod_re * back_enter_re + prod_im * back_enter_im
    adjoint_im = adjoint_im + prod_re * back_enter_im - prod_im * back_enter_re
    return (state_re, state_im, adjoint_re, adjoint_im)


def rms_normed(block_in, norm_gain):
    widened = block_in.astype(F32)
    spread = jnp.mean(widened * widened, axis=1, keepdims=True)
    return widened, (widened * lax.rsqrt(spread + epsilon) * norm_gain).astype(BF16)


def body_any(tokens, token_ids, norm_gain, w_in, rates, phases, forget, readout, skip, out_grad):
    block_ids = token_ids[0]
    block_grad = out_grad[0]
    pairs = rates.shape[0]
    widened, normed = rms_normed(tokens[0], norm_gain)
    inputs = jnp.dot(
        normed, lax.all_gather(w_in, "fsdp", axis=0, tiled=True), preferred_element_type=F32
    )
    radius = jnp.exp(-rates)
    in_scale = jnp.sqrt(-jnp.expm1(-2.0 * rates))
    up_re = readout[0]
    up_im = readout[1]
    retain = jnp.where(block_ids[:, None] >= first_special, 1.0 - forget[None, :], 1.0)
    decay_re = retain * radius * jnp.cos(phases)
    decay_im = retain * radius * jnp.sin(phases)
    drive_re = in_scale * inputs[:, :pairs]
    drive_im = in_scale * inputs[:, pairs:]
    grad_wide = block_grad.astype(F32)
    state_re = up_re * grad_wide[:, :pairs] + up_im * grad_wide[:, pairs:]
    state_im = up_re * grad_wide[:, pairs:] - up_im * grad_wide[:, :pairs]
    back_re = decay_re * state_re + decay_im * state_im
    back_im = decay_re * state_im - decay_im * state_re
    elements = (decay_re, decay_im, drive_re, drive_im, back_re, back_im)
    ahead = lax.associative_scan(chain_join, elements, axis=0)
    behind = lax.associative_scan(chain_join, elements, reverse=True, axis=0)
    ahead_summary = tuple((member[-1] for member in ahead))
    behind_summary = tuple((member[0] for member in behind))
    ones_row = jnp.ones((pairs,), F32)
    zeros_row = jnp.zeros((pairs,), F32)
    identity = (ones_row, zeros_row, zeros_row, zeros_row, zeros_row, zeros_row)
    ahead_in = carried_in(ahead_summary, "seq", chain_join, identity, False)
    behind_in = carried_in(behind_summary, "seq", chain_join, identity, True)
    fwd_re, fwd_im, sigma_re, sigma_im = apply_carry(ahead, ahead_in)
    bwd_re, bwd_im, rho_re, rho_im = apply_carry(behind, behind_in)
    sum_re = fwd_re + bwd_re
    sum_im = fwd_im + bwd_im
    out_re = up_re * sum_re - up_im * sum_im
    out_im = up_re * sum_im + up_im * sum_re
    branch = jnp.concatenate([out_re, out_im], axis=1)
    mixed = (widened + branch + skip * normed.astype(F32)).astype(BF16)
    later_re = jnp.concatenate([rho_re[1:], behind_in[4][None, :]], axis=0)
    later_im = jnp.concatenate([rho_im[1:], behind_in[5][None, :]], axis=0)
    former_re = jnp.concatenate([ahead_in[4][None, :], sigma_re[:-1]], axis=0)
    former_im = jnp.concatenate([ahead_in[5][None, :], sigma_im[:-1]], axis=0)
    grad_re = in_scale * (2.0 * state_re + later_re + former_re)
    grad_im = in_scale * (2.0 * state_im + later_im + former_im)
    input_grad = jnp.concatenate([grad_re, grad_im], axis=1).astype(BF16)
    row_block = lax.psum_scatter(
        lax.dot_general(
            normed, input_grad, (((0,), (0,)), ((), ())), preferred_element_type=F32
        ),
        "fsdp",
        scatter_dimension=0,
        tiled=True,
    )
    grad_w_in = lax.psum_scatter(row_block, "seq", scatter_dimension=1, tiled=True)
    return (mixed[None], grad_w_in)


SLAB = ("x", "y", "c")
PIECES = 4
FIRST, SECOND = (3, 2), (1, 0)
PLACES = [(k % 2, k // 2 % 2, k // 4) for k in range(8)]
CUT_PLACES = [place for place in PLACES for _ in range(1 + place[0] * place[1])]


def flip(value, *axes):
    count = 2 ** len(axes)
    return lax.ppermute(value, axes, [(i, count - 1 - i) for i in range(count)])


def z_flip(value, distance, count):
    return lax.ppermute(value, "z", [(i, i ^ distance) for i in range(count)])


def exchange(value, axes):
    return lax.all_to_all(value, axes, 0, 0, tiled=True)


def cmul(a_re, a_im, b_re, b_im):
    return a_re * b_re - a_im * b_im, a_re * b_im + a_im * b_re


def iota(shape, dim):
    return lax.broadcasted_iota(jnp.int32, shape, dim)


def reorder(half, back=False):
    steps = half // ROWS
    row, position = iota((half, half), int(back)), iota((half, half), 1 - int(back))
    hit = position == lax.rem(row, ROWS) * steps + lax.div(row, ROWS)
    return jnp.where(hit, 1.0, 0.0).astype(BF16)


def cut_kernel(w, *outs):
    wide = outs[0].shape[1] // 2
    for d, out in enumerate(outs):
        dy, dc = divmod(d, 2)
        here = positions()
        to = (here["x"] * 2 + (here["y"] ^ dy)) * 2 + (here["c"] ^ dc)
        for part in range(2):
            columns = pl.ds(pl.multiple_of(to * wide + part * (w.shape[1] // 2), wide), wide)
            out[:, part * wide : (part + 1) * wide] = w[:, columns]


def stack_kernel(*refs):
    pieces, out = refs[:-1], refs[-1]
    here = positions()
    for d, piece in enumerate(pieces):
        dy, dc = divmod(d, 2)
        out[(here["y"] ^ dy) * 2 + (here["c"] ^ dc)] = piece[...]


def rms_rows(tokens, gain):
    widened = tokens.astype(F32)
    spread = jnp.mean(widened * widened, axis=1, keepdims=True)
    return widened, (widened * lax.rsqrt(spread + epsilon) * gain).astype(BF16)


def norm_kernel(tokens, gain, first, second, rows, held, done):
    copy = pltpu.make_async_copy(tokens, rows, done)
    copy.start()
    copy.wait()
    _, normed = rms_rows(rows[0], gain[...])
    held[...] = jnp.dot(reorder(held.shape[0]), normed, preferred_element_type=F32).astype(BF16)
    width = first.shape[1] // 2
    for out, distances in ((first, FIRST), (second, SECOND)):
        for k, dz in enumerate(distances):
            at = pl.multiple_of((positions()["z"] ^ dz) * width, width)
            out[:, k * width : (k + 1) * width] = held[:, pl.ds(at, width)]


def grad_kernel(grad, ids, out):
    members, rows, both = out.shape
    half, wide = grad.shape[1], both // 2
    steps = half // ROWS
    moved = jnp.dot(reorder(half), grad[0], preferred_element_type=F32).astype(BF16)
    special = jnp.where(ids[...] >= first_special, 1.0, 0.0).astype(F32)
    under = (rows - half, half)
    spread = jnp.where(lax.div(iota(under, 1), steps) == iota(under, 0), special, 0.0).astype(BF16)
    pick = jnp.where(lax.rem(iota((half, both), 0), steps) == iota((half, both), 1), 1.0, 0.0)
    flags = jnp.dot(spread, pick.astype(BF16), preferred_element_type=F32).astype(BF16)
    for m in range(members):
        for part in range(2):
            at = (part * members + m) * wide
            out[m, :half, part * wide : (part + 1) * wide] = moved[:, at : at + wide]
        out[m, half:, :] = flags


def scan_chunks(x_re, x_im, p_re, p_im, backward):
    rows = iota(x_re.shape, 0)

    def moved(value, by, fill):
        if backward:
            return jnp.where(rows < ROWS - by, pltpu.roll(value, ROWS - by, 0), fill)
        return jnp.where(rows >= by, pltpu.roll(value, by, 0), fill)

    by = 1
    while by < ROWS:
        add_re, add_im = cmul(p_re, p_im, moved(x_re, by, 0.0), moved(x_im, by, 0.0))
        p_re, p_im = cmul(p_re, p_im, moved(p_re, by, 1.0), moved(p_im, by, 0.0))
        x_re, x_im = x_re + add_re, x_im + add_im
        by *= 2
    end = 0 if backward else ROWS - 1
    total = (x_re[end : end + 1, :], x_im[end : end + 1, :])
    enter = (moved(x_re, 1, 0.0), moved(x_im, 1, 0.0))
    decay = (moved(p_re, 1, 1.0), moved(p_im, 1, 0.0))
    return total, enter, decay


def both_ways(adjoint, group, pars, keep, val, res):
    blocks, steps, _, wide = keep.shape
    count = blocks // 2
    lam_re = jnp.broadcast_to(pars[0:1, :], (ROWS, wide))
    lam_im = jnp.broadcast_to(pars[1:2, :], (ROWS, wide))
    if adjoint:
        lam_im = -lam_im
    pow_re, pow_im = lam_re, lam_im
    done = 1
    while done < steps:
        pow_re, pow_im = cmul(pow_re, pow_im, pow_re, pow_im)
        done *= 2
    zero = jnp.zeros((ROWS, wide), F32)

    def step(m, j, state):
        held, v_re, v_im = keep[m, j], val[0, m, j], val[1, m, j]
        if adjoint:
            out = (v_re + state[0], v_im + state[1])
            n_re, n_im = cmul(lam_re, lam_im, *out)
            return (held * n_re, held * n_im), out
        n_re, n_im = cmul(lam_re, lam_im, held * state[0], held * state[1])
        n_re, n_im = n_re + v_re, n_im + v_im
        return (n_re, n_im), (n_re, n_im)

    for first in range(0, count, group):
        chains = [x * count + q for q in range(first, first + group) for x in range(2)]
        ahead = {m: (zero, zero) for m in chains}
        behind = {m: (zero, zero) for m in chains}
        kept = {m: zero + 1.0 for m in chains}
        for i in range(steps):
            for m in chains:
                ahead[m], _ = step(m, i, ahead[m])
                behind[m], _ = step(m, steps - 1 - i, behind[m])
                kept[m] = kept[m] * keep[m, i]
        for q in range(first, first + group):
            for states, order, backward in ((ahead, (q, count + q), False), (behind, (count + q, q), True)):
                near, far = order
                total, enter, _ = scan_chunks(
                    *states[near], kept[near] * pow_re, kept[near] * pow_im, backward
                )
                _, later, decay = scan_chunks(
                    *states[far], kept[far] * pow_re, kept[far] * pow_im, backward
                )
                add_re, add_im = cmul(*decay, *total)
                states[near] = enter
                states[far] = (later[0] + add_re, later[1] + add_im)
        for i in range(steps):
            for m in chains:
                ahead[m], out_a = step(m, i, ahead[m])
                behind[m], out_b = step(m, steps - 1 - i, behind[m])
                for part in range(2):
                    if i < steps // 2:
                        res[part, m, i] = out_a[part]
                        res[part, m, steps - 1 - i] = out_b[part]
                    else:
                        res[part, m, i] = res[part, m, i] + out_a[part]
                        res[part, m, steps - 1 - i] = res[part, m, steps - 1 - i] + out_b[part]


def fill_keep(m, chunk, pars, keep):
    steps = keep.shape[1]
    lose = jnp.broadcast_to(pars[2:3, :], keep.shape[-2:])
    for j in range(steps):
        keep[m, j] = 1.0 - jnp.broadcast_to(chunk[:, j : j + 1], lose.shape) * lose


def adjoint_kernel(og, pars, ig, flags, keep, val, res):
    blocks, steps, _, wide = keep.shape
    half = steps * ROWS
    shape = (steps, ROWS, wide)
    c_re, c_im = pars[3:4, :], pars[4:5, :]
    for m in range(blocks):
        chunk = og[m, half:, :].astype(F32)[:ROWS, :wide]
        flags[m] = chunk
        fill_keep(m, chunk, pars, keep)
        q_re = og[m, :half, :wide].astype(F32)
        q_im = og[m, :half, wide:].astype(F32)
        val[0, m] = (c_re * q_re + c_im * q_im).reshape(shape)
        val[1, m] = (c_re * q_im - c_im * q_re).reshape(shape)
    both_ways(True, 2, pars, keep, val, res)
    for m in range(blocks):
        for part in range(2):
            block = res[part, m].reshape(half, wide)
            ig[part * wide : (part + 1) * wide, m * half : (m + 1) * half] = block.T.astype(BF16)


def pack(pieces, here, out, columns=slice(None)):
    half = out.shape[1]
    starts = {}
    for piece, (dx, dy, dc) in zip(pieces, CUT_PLACES):
        m = ((here["x"] ^ dx) * 2 + (here["y"] ^ dy)) * 2 + (here["c"] ^ dc)
        start = starts.get((dx, dy, dc), 0)
        starts[dx, dy, dc] = stop = start + piece.shape[0]
        out[m, start % half : start % half + piece.shape[0], columns] = piece[...]
        assert stop <= half


def positions():
    return {axis: lax.axis_index(axis) for axis in ("x", "z", "y", "c")}


def forward_kernel(*refs):
    count = len(CUT_PLACES)
    first, second, refs = refs[:count], refs[count : 2 * count], refs[2 * count :]
    wbs, refs = refs[:4], refs[4:]
    flags, pars, branch, n_all, w_all, keep, val, res = refs
    blocks, steps, _, wide = keep.shape
    half = steps * ROWS
    here = positions()
    for k, dz in enumerate(FIRST + SECOND):
        w_all[k] = wbs[dz][...].reshape(w_all.shape[1:])
    middle = n_all.shape[2] // 2
    pack(first, here, n_all, slice(0, middle))
    pack(second, here, n_all, slice(middle, 2 * middle))
    for m in range(blocks):
        fill_keep(m, flags[m], pars, keep)
    model = n_all.shape[2]
    got = jnp.dot(
        n_all[...].reshape(blocks * half, model),
        w_all[...].reshape(model, 2 * wide),
        preferred_element_type=F32,
    )
    val[0] = got[:, :wide].reshape(blocks, steps, ROWS, wide)
    val[1] = got[:, wide:].reshape(blocks, steps, ROWS, wide)
    both_ways(False, 2, pars, keep, val, res)
    c_re, c_im = pars[3:4, :], pars[4:5, :]
    for m in range(blocks):
        s_re = res[0, m].reshape(half, wide)
        s_im = res[1, m].reshape(half, wide)
        branch[m, :, :wide] = (c_re * s_re - c_im * s_im).astype(BF16)
        branch[m, :, wide:] = (c_re * s_im + c_im * s_re).astype(BF16)


def outer_kernel(*refs):
    pieces, refs = refs[: len(CUT_PLACES)], refs[len(CUT_PLACES) :]
    ig, outs, n_cut = refs[0], refs[1:-1], refs[-1]
    blocks, half, _ = n_cut.shape
    pack(pieces, positions(), n_cut)
    across = outs[0].shape[1]
    for k, out in enumerate(outs):
        rows = n_cut[:, :, k * across : (k + 1) * across].reshape(blocks * half, across)
        out[...] = jnp.dot(ig[...], rows, preferred_element_type=F32).astype(out.dtype)


def flipped(here, place):
    x, y, c = (here[axis] ^ bit for axis, bit in zip(SLAB, place))
    return (x * 2 + y) * 2 + c, x, y * 2 + c


def pre_kernel(own, other, out):
    out[...] = own[...] + other[...].astype(F32)


def sum_kernel(count, *refs):
    sent, outs, held = refs[:count], refs[count:-count - 2], refs[-count - 2 : -2]
    total, done = refs[-2:]
    copies = [pltpu.make_async_copy(src, dst, done.at[k]) for k, (src, dst) in enumerate(zip(sent, held))]
    for copy in copies:
        copy.start()
    for copy in copies:
        copy.wait()
    _, rows, wide = outs[0].shape
    got = held[0][...]
    for other in held[1:]:
        got = got + other[...].astype(F32)
    total[...] = got
    here = positions()
    for k, place in enumerate(PLACES):
        _, part, d = flipped(here, place)
        at = pl.ds(pl.multiple_of(part * wide, wide), wide)
        columns = pl.ds(pl.multiple_of(d * rows, rows), rows)
        outs[place[2]][k % 4] = total[at, columns].T.astype(BF16)


def pair_kernel(same, came, *outs):
    for k, out in enumerate(outs):
        out[0] = same[k]
        out[1] = came[k]


def place_kernel(*refs):
    got, out = refs[:-1], refs[-1]
    here = positions()
    for (dx, dy, dc), block in zip(PLACES, [block.at[c] for c in (0, 1) for block in got]):
        m, _, _ = flipped(here, (dx, dy, dc))
        wide = block.shape[1]
        out[:, pl.ds(pl.multiple_of(m * wide, wide), wide)] = block[...].astype(F32)


def mixed_kernel(tokens, gain, skip, branch, out):
    members, half, both = branch.shape
    wide = both // 2
    widened, normed = rms_rows(tokens[0], gain[...])
    base = widened + skip[...] * normed.astype(F32)
    back = reorder(half, True)
    for m in range(members):
        got = jnp.dot(back, branch[m], preferred_element_type=F32)
        for part in range(2):
            columns = slice((part * members + m) * wide, (part * members + m + 1) * wide)
            total = base[:, columns] + got[:, part * wide : (part + 1) * wide]
            out[0, :, columns] = total.astype(BF16)


def call(kernel, out_shape, inputs, scratch=(), mib=8, flops=1_000_000, spaces=None):
    vmem = pl.BlockSpec(memory_space=pltpu.VMEM)
    made = jax.tree.leaves(out_shape)
    moved = sum(a.size * a.dtype.itemsize for a in [*inputs, *made])
    return pl.pallas_call(
        kernel,
        out_shape=out_shape,
        in_specs=[pl.BlockSpec(memory_space=space) for space in spaces or [pltpu.VMEM] * len(inputs)],
        out_specs=jax.tree.map(lambda _: vmem, out_shape),
        scratch_shapes=list(scratch),
        compiler_params=pltpu.CompilerParams(vmem_limit_bytes=mib * 2**20),
        cost_estimate=pl.CostEstimate(flops=flops, bytes_accessed=moved, transcendentals=0),
    )(*inputs)


def body_slab(layout, *inputs):
    return slab_step(layout, *inputs)


def slab_step(layout, tokens, token_ids, norm_gain, w_in, rates, phases, forget, readout, skip, out_grad):
    half, model = tokens.shape[1:]
    pairs = rates.shape[0]
    n_z, count = layout["z"], PIECES
    members = 2 * count
    wide = pairs // members
    steps = half // ROWS
    mine = (lax.axis_index("x") * 2 + lax.axis_index("y")) * 2 + lax.axis_index("c")

    def shaped(shape, dtype=BF16):
        return jax.ShapeDtypeStruct(shape, dtype)

    w_cut = call(cut_kernel, [shaped((w_in.shape[0], 2 * wide))] * count, [w_in])
    w_cut = list(w_cut)
    w_cut[1] = flip(w_cut[1], "c")
    w_cut[2] = flip(w_cut[2], "y")
    w_cut[3] = flip(w_cut[3], "y", "c")
    w_own = call(stack_kernel, shaped((count, w_in.shape[0], 2 * wide)), w_cut)
    w_2 = z_flip(w_own, 2, n_z)
    w_1 = z_flip(w_own, 1, n_z)
    w_3 = z_flip(w_2, 1, n_z)

    gain = norm_gain.reshape(1, model)
    first, second = call(
        norm_kernel,
        [shaped((half, model // 2))] * 2,
        [tokens, gain],
        [pltpu.VMEM(tokens.shape, BF16), pltpu.VMEM((half, model), BF16), pltpu.SemaphoreType.DMA],
        spaces=[pl.ANY, pltpu.VMEM],
    )
    first = [first, flip(first, "x"), flip(first, "y")]
    first += [flip(first[2][: half // 2], "x"), flip(first[1][half // 2 :], "y")]
    second = [second, flip(second, "x"), flip(second, "y")]
    second += [flip(second[2][: half // 2], "x"), flip(second[1][half // 2 :], "y")]
    first += [flip(piece, "c") for piece in first]
    second += [flip(piece, "c") for piece in second]

    under = 16
    og = call(grad_kernel, shaped((members, half + under, 2 * wide)), [out_grad, token_ids])
    og = exchange(og, SLAB)

    radius = jnp.exp(-rates)
    in_scale = jnp.sqrt(-jnp.expm1(-2.0 * rates))
    rows = [radius * jnp.cos(phases), radius * jnp.sin(phases), forget, in_scale * readout[0], in_scale * readout[1]]
    rows = jnp.stack(rows + [jnp.zeros_like(rates)] * (ROWS - len(rows)))
    pars = lax.dynamic_slice_in_dim(rows, mine * wide, wide, axis=1)

    chains = [
        pltpu.VMEM((members, steps, ROWS, wide), F32),
        pltpu.VMEM((2, members, steps, ROWS, wide), F32),
        pltpu.VMEM((2, members, steps, ROWS, wide), F32),
    ]
    ig, flags = call(
        adjoint_kernel,
        [shaped((2 * wide, members * half)), shaped((members, ROWS, wide), F32)],
        [og, pars],
        chains,
        flops=20_000_000,
    )

    across = model // n_z
    matmul = 2 * members * half * model * 2 * wide
    parts = {}
    for pieces, distances in ((first, FIRST), (second, SECOND)):
        made = call(
            outer_kernel,
            [shaped((2 * wide, across), BF16 if dz else F32) for dz in distances],
            [*pieces, ig],
            [pltpu.VMEM((members, half, model // 2), BF16)],
            mib=16,
            flops=matmul // 2,
        )
        parts.update(zip(distances, made))
    got = [z_flip(parts[dz], dz, n_z) for dz in (3, 2, 1)]

    branch = call(
        forward_kernel,
        shaped((members, half, 2 * wide)),
        [*first, *second, w_own, w_1, w_2, w_3, flags, pars],
        [pltpu.VMEM((members, half, model), BF16), pltpu.VMEM((n_z, model // n_z, 2 * wide), BF16)] + chains,
        mib=24,
        flops=matmul,
    )
    branch = exchange(branch, SLAB)
    mixed = call(
        mixed_kernel, shaped(tokens.shape), [tokens, gain, skip.reshape(1, model), branch], flops=10_000_000
    )

    early = call(pre_kernel, shaped((2 * wide, across), F32), [parts[0], got[0]])
    sums = [early, *got[1:]]
    total = call(
        functools.partial(sum_kernel, len(sums)),
        [shaped((count, across // count, wide))] * 2,
        sums,
        [
            *(pltpu.VMEM(part.shape, part.dtype) for part in sums),
            pltpu.VMEM((2 * wide, across), F32),
            pltpu.SemaphoreType.DMA((len(sums),)),
        ],
        mib=8,
        spaces=[pl.ANY] * len(sums),
    )
    same, other = total
    came = flip(other, "c")
    pairs_of = call(pair_kernel, [shaped((2, across // count, wide))] * count, [same, came])
    placed = [
        pairs_of[0], flip(pairs_of[1], "x"), flip(pairs_of[2], "y"), flip(pairs_of[3], "x", "y")
    ]
    grad_w_in = call(place_kernel, shaped((across // count, pairs), F32), placed)
    return (mixed, grad_w_in)


def solution(mesh):
    n_seq, n_fsdp = mesh.shape["seq"], mesh.shape["fsdp"]
    if n_seq == 2 and n_fsdp == 16:
        layout = {"x": n_seq, "z": n_fsdp // 4, "y": 2, "c": 2}
        mesh = Mesh(mesh.devices.reshape(tuple(layout.values())), tuple(layout))
        body, fsdp, seq = functools.partial(body_slab, layout), ("z", "y", "c"), "x"
    else:
        body, fsdp, seq = body_any, "fsdp", "seq"
    in_specs = (
        P(fsdp, seq, None),
        P(fsdp, seq),
        P(),
        P(fsdp, None),
        P(),
        P(),
        P(),
        P(),
        P(),
        P(fsdp, seq, None),
    )
    out_specs = (P(fsdp, seq, None), P(fsdp, seq))
    step = jax.shard_map(body, mesh=mesh, in_specs=in_specs, out_specs=out_specs, check_vma=False)
    if body is body_any:
        return step
    return step
```

```python
import functools

import jax
import jax.numpy as jnp
from jax import lax
from jax.experimental import pallas as pl
from jax.experimental.pallas import tpu as pltpu
from jax.sharding import Mesh, PartitionSpec as P


epsilon = 1e-06
first_special = 4
ROWS = 8
BF16 = jnp.bfloat16
F32 = jnp.float32


def carried_in(value, axis, join, neutral, backward):
    count, mine = (lax.axis_size(axis), lax.axis_index(axis))
    pieces = jax.tree.map(lambda part: lax.all_gather(part, axis), value)
    if backward:
        pieces = jax.tree.map(lambda part: part[::-1], pieces)
        mine = count - 1 - mine
    running = jax.tree.map(
        lambda part, zero: jnp.full_like(part, 0) + jnp.asarray(zero, part.dtype), value, neutral
    )

    def turn(position, running):
        longer = join(running, jax.tree.map(lambda part: part[position], pieces))
        return jax.tree.map(lambda new, old: jnp.where(position < mine, new, old), longer, running)

    return lax.fori_loop(0, count - 1, turn, running)


def chain_join(earlier, later):
    a_re, a_im, b_re, b_im, c_re, c_im = earlier
    p_re, p_im, q_re, q_im, s_re, s_im = later
    return (
        p_re * a_re - p_im * a_im,
        p_re * a_im + p_im * a_re,
        p_re * b_re - p_im * b_im + q_re,
        p_re * b_im + p_im * b_re + q_im,
        p_re * c_re + p_im * c_im + s_re,
        p_re * c_im - p_im * c_re + s_im,
    )


def apply_carry(local, carry):
    prod_re, prod_im, state_re, state_im, adjoint_re, adjoint_im = local
    enter_re = carry[2][None, :]
    enter_im = carry[3][None, :]
    back_enter_re = carry[4][None, :]
    back_enter_im = carry[5][None, :]
    state_re = state_re + prod_re * enter_re - prod_im * enter_im
    state_im = state_im + prod_re * enter_im + prod_im * enter_re
    adjoint_re = adjoint_re + prod_re * back_enter_re + prod_im * back_enter_im
    adjoint_im = adjoint_im + prod_re * back_enter_im - prod_im * back_enter_re
    return (state_re, state_im, adjoint_re, adjoint_im)


def rms_normed(block_in, norm_gain):
    widened = block_in.astype(F32)
    spread = jnp.mean(widened * widened, axis=1, keepdims=True)
    return widened, (widened * lax.rsqrt(spread + epsilon) * norm_gain).astype(BF16)


def body_any(tokens, token_ids, norm_gain, w_in, rates, phases, forget, readout, skip, out_grad):
    block_ids = token_ids[0]
    block_grad = out_grad[0]
    pairs = rates.shape[0]
    widened, normed = rms_normed(tokens[0], norm_gain)
    inputs = jnp.dot(
        normed, lax.all_gather(w_in, "fsdp", axis=0, tiled=True), preferred_element_type=F32
    )
    radius = jnp.exp(-rates)
    in_scale = jnp.sqrt(-jnp.expm1(-2.0 * rates))
    up_re = readout[0]
    up_im = readout[1]
    retain = jnp.where(block_ids[:, None] >= first_special, 1.0 - forget[None, :], 1.0)
    decay_re = retain * radius * jnp.cos(phases)
    decay_im = retain * radius * jnp.sin(phases)
    drive_re = in_scale * inputs[:, :pairs]
    drive_im = in_scale * inputs[:, pairs:]
    grad_wide = block_grad.astype(F32)
    state_re = up_re * grad_wide[:, :pairs] + up_im * grad_wide[:, pairs:]
    state_im = up_re * grad_wide[:, pairs:] - up_im * grad_wide[:, :pairs]
    back_re = decay_re * state_re + decay_im * state_im
    back_im = decay_re * state_im - decay_im * state_re
    elements = (decay_re, decay_im, drive_re, drive_im, back_re, back_im)
    ahead = lax.associative_scan(chain_join, elements, axis=0)
    behind = lax.associative_scan(chain_join, elements, reverse=True, axis=0)
    ahead_summary = tuple((member[-1] for member in ahead))
    behind_summary = tuple((member[0] for member in behind))
    ones_row = jnp.ones((pairs,), F32)
    zeros_row = jnp.zeros((pairs,), F32)
    identity = (ones_row, zeros_row, zeros_row, zeros_row, zeros_row, zeros_row)
    ahead_in = carried_in(ahead_summary, "seq", chain_join, identity, False)
    behind_in = carried_in(behind_summary, "seq", chain_join, identity, True)
    fwd_re, fwd_im, sigma_re, sigma_im = apply_carry(ahead, ahead_in)
    bwd_re, bwd_im, rho_re, rho_im = apply_carry(behind, behind_in)
    sum_re = fwd_re + bwd_re
    sum_im = fwd_im + bwd_im
    out_re = up_re * sum_re - up_im * sum_im
    out_im = up_re * sum_im + up_im * sum_re
    branch = jnp.concatenate([out_re, out_im], axis=1)
    mixed = (widened + branch + skip * normed.astype(F32)).astype(BF16)
    later_re = jnp.concatenate([rho_re[1:], behind_in[4][None, :]], axis=0)
    later_im = jnp.concatenate([rho_im[1:], behind_in[5][None, :]], axis=0)
    former_re = jnp.concatenate([ahead_in[4][None, :], sigma_re[:-1]], axis=0)
    former_im = jnp.concatenate([ahead_in[5][None, :], sigma_im[:-1]], axis=0)
    grad_re = in_scale * (2.0 * state_re + later_re + former_re)
    grad_im = in_scale * (2.0 * state_im + later_im + former_im)
    input_grad = jnp.concatenate([grad_re, grad_im], axis=1).astype(BF16)
    row_block = lax.psum_scatter(
        lax.dot_general(
            normed, input_grad, (((0,), (0,)), ((), ())), preferred_element_type=F32
        ),
        "fsdp",
        scatter_dimension=0,
        tiled=True,
    )
    grad_w_in = lax.psum_scatter(row_block, "seq", scatter_dimension=1, tiled=True)
    return (mixed[None], grad_w_in)


SLAB = ("x", "y", "c")
PIECES = 4
FIRST, SECOND = (3, 2), (1, 0)
PLACES = [(k % 2, k // 2 % 2, k // 4) for k in range(8)]
CUT_PLACES = [place for place in PLACES for _ in range(1 + place[0] * place[1])]


def flip(value, *axes):
    count = 2 ** len(axes)
    return lax.ppermute(value, axes, [(i, count - 1 - i) for i in range(count)])


def z_flip(value, distance, count):
    return lax.ppermute(value, "z", [(i, i ^ distance) for i in range(count)])


def exchange(value, axes):
    return lax.all_to_all(value, axes, 0, 0, tiled=True)


def cmul(a_re, a_im, b_re, b_im):
    return a_re * b_re - a_im * b_im, a_re * b_im + a_im * b_re


def iota(shape, dim):
    return lax.broadcasted_iota(jnp.int32, shape, dim)


def reorder(half, back=False):
    steps = half // ROWS
    row, position = iota((half, half), int(back)), iota((half, half), 1 - int(back))
    hit = position == lax.rem(row, ROWS) * steps + lax.div(row, ROWS)
    return jnp.where(hit, 1.0, 0.0).astype(BF16)


def cut_kernel(w, *outs):
    wide = outs[0].shape[1] // 2
    for d, out in enumerate(outs):
        dy, dc = divmod(d, 2)
        here = positions()
        to = (here["x"] * 2 + (here["y"] ^ dy)) * 2 + (here["c"] ^ dc)
        for part in range(2):
            columns = pl.ds(pl.multiple_of(to * wide + part * (w.shape[1] // 2), wide), wide)
            out[:, part * wide : (part + 1) * wide] = w[:, columns]


def stack_kernel(*refs):
    pieces, out = refs[:-1], refs[-1]
    here = positions()
    for d, piece in enumerate(pieces):
        dy, dc = divmod(d, 2)
        out[(here["y"] ^ dy) * 2 + (here["c"] ^ dc)] = piece[...]


def rms_rows(tokens, gain):
    widened = tokens.astype(F32)
    spread = jnp.mean(widened * widened, axis=1, keepdims=True)
    return widened, (widened * lax.rsqrt(spread + epsilon) * gain).astype(BF16)


def norm_kernel(tokens, gain, first, second, rows, held, done):
    copy = pltpu.make_async_copy(tokens, rows, done)
    copy.start()
    copy.wait()
    _, normed = rms_rows(rows[0], gain[...])
    held[...] = jnp.dot(reorder(held.shape[0]), normed, preferred_element_type=F32).astype(BF16)
    width = first.shape[1] // 2
    for out, distances in ((first, FIRST), (second, SECOND)):
        for k, dz in enumerate(distances):
            at = pl.multiple_of((positions()["z"] ^ dz) * width, width)
            out[:, k * width : (k + 1) * width] = held[:, pl.ds(at, width)]


def halve_kernel(over_y, over_x, top, bottom):
    rows = top.shape[0]
    top[...] = over_y[:rows]
    bottom[...] = over_x[rows:]


def grad_kernel(grad, ids, out):
    members, rows, both = out.shape
    half, wide = grad.shape[1], both // 2
    steps = half // ROWS
    moved = jnp.dot(reorder(half), grad[0], preferred_element_type=F32).astype(BF16)
    special = jnp.where(ids[...] >= first_special, 1.0, 0.0).astype(F32)
    under = (rows - half, half)
    spread = jnp.where(lax.div(iota(under, 1), steps) == iota(under, 0), special, 0.0).astype(BF16)
    pick = jnp.where(lax.rem(iota((half, both), 0), steps) == iota((half, both), 1), 1.0, 0.0)
    flags = jnp.dot(spread, pick.astype(BF16), preferred_element_type=F32).astype(BF16)
    for m in range(members):
        for part in range(2):
            at = (part * members + m) * wide
            out[m, :half, part * wide : (part + 1) * wide] = moved[:, at : at + wide]
        out[m, half:, :] = flags


def scan_chunks(x_re, x_im, p_re, p_im, backward):
    rows = iota(x_re.shape, 0)

    def moved(value, by, fill):
        if backward:
            return jnp.where(rows < ROWS - by, pltpu.roll(value, ROWS - by, 0), fill)
        return jnp.where(rows >= by, pltpu.roll(value, by, 0), fill)

    by = 1
    while by < ROWS:
        add_re, add_im = cmul(p_re, p_im, moved(x_re, by, 0.0), moved(x_im, by, 0.0))
        p_re, p_im = cmul(p_re, p_im, moved(p_re, by, 1.0), moved(p_im, by, 0.0))
        x_re, x_im = x_re + add_re, x_im + add_im
        by *= 2
    end = 0 if backward else ROWS - 1
    total = (x_re[end : end + 1, :], x_im[end : end + 1, :])
    enter = (moved(x_re, 1, 0.0), moved(x_im, 1, 0.0))
    decay = (moved(p_re, 1, 1.0), moved(p_im, 1, 0.0))
    return total, enter, decay


def both_ways(adjoint, group, pars, keep, val, res):
    blocks, steps, _, wide = keep.shape
    count = blocks // 2
    lam_re = jnp.broadcast_to(pars[0:1, :], (ROWS, wide))
    lam_im = jnp.broadcast_to(pars[1:2, :], (ROWS, wide))
    if adjoint:
        lam_im = -lam_im
    pow_re, pow_im = lam_re, lam_im
    done = 1
    while done < steps:
        pow_re, pow_im = cmul(pow_re, pow_im, pow_re, pow_im)
        done *= 2
    zero = jnp.zeros((ROWS, wide), F32)

    def step(m, j, state):
        held, v_re, v_im = keep[m, j], val[0, m, j], val[1, m, j]
        if adjoint:
            out = (v_re + state[0], v_im + state[1])
            n_re, n_im = cmul(lam_re, lam_im, *out)
            return (held * n_re, held * n_im), out
        n_re, n_im = cmul(lam_re, lam_im, held * state[0], held * state[1])
        n_re, n_im = n_re + v_re, n_im + v_im
        return (n_re, n_im), (n_re, n_im)

    for first in range(0, count, group):
        chains = [x * count + q for q in range(first, first + group) for x in range(2)]
        ahead = {m: (zero, zero) for m in chains}
        behind = {m: (zero, zero) for m in chains}
        kept = {m: zero + 1.0 for m in chains}
        for i in range(steps):
            for m in chains:
                ahead[m], _ = step(m, i, ahead[m])
                behind[m], _ = step(m, steps - 1 - i, behind[m])
                kept[m] = kept[m] * keep[m, i]
        for q in range(first, first + group):
            for states, order, backward in ((ahead, (q, count + q), False), (behind, (count + q, q), True)):
                near, far = order
                total, enter, _ = scan_chunks(
                    *states[near], kept[near] * pow_re, kept[near] * pow_im, backward
                )
                _, later, decay = scan_chunks(
                    *states[far], kept[far] * pow_re, kept[far] * pow_im, backward
                )
                add_re, add_im = cmul(*decay, *total)
                states[near] = enter
                states[far] = (later[0] + add_re, later[1] + add_im)
        for i in range(steps):
            for m in chains:
                ahead[m], out_a = step(m, i, ahead[m])
                behind[m], out_b = step(m, steps - 1 - i, behind[m])
                for part in range(2):
                    if i < steps // 2:
                        res[part, m, i] = out_a[part]
                        res[part, m, steps - 1 - i] = out_b[part]
                    else:
                        res[part, m, i] = res[part, m, i] + out_a[part]
                        res[part, m, steps - 1 - i] = res[part, m, steps - 1 - i] + out_b[part]


def fill_keep(m, chunk, pars, keep):
    steps = keep.shape[1]
    lose = jnp.broadcast_to(pars[2:3, :], keep.shape[-2:])
    for j in range(steps):
        keep[m, j] = 1.0 - jnp.broadcast_to(chunk[:, j : j + 1], lose.shape) * lose


def adjoint_kernel(og, pars, ig, flags, keep, val, res):
    blocks, steps, _, wide = keep.shape
    half = steps * ROWS
    shape = (steps, ROWS, wide)
    c_re, c_im = pars[3:4, :], pars[4:5, :]
    for m in range(blocks):
        chunk = og[m, half:, :].astype(F32)[:ROWS, :wide]
        flags[m] = chunk
        fill_keep(m, chunk, pars, keep)
        q_re = og[m, :half, :wide].astype(F32)
        q_im = og[m, :half, wide:].astype(F32)
        val[0, m] = (c_re * q_re + c_im * q_im).reshape(shape)
        val[1, m] = (c_re * q_im - c_im * q_re).reshape(shape)
    both_ways(True, 2, pars, keep, val, res)
    for m in range(blocks):
        for part in range(2):
            block = res[part, m].reshape(half, wide)
            ig[part * wide : (part + 1) * wide, m * half : (m + 1) * half] = block.T.astype(BF16)


def pack(pieces, here, out, columns=slice(None)):
    half = out.shape[1]
    starts = {}
    for piece, (dx, dy, dc) in zip(pieces, CUT_PLACES):
        m = ((here["x"] ^ dx) * 2 + (here["y"] ^ dy)) * 2 + (here["c"] ^ dc)
        start = starts.get((dx, dy, dc), 0)
        starts[dx, dy, dc] = stop = start + piece.shape[0]
        out[m, start % half : start % half + piece.shape[0], columns] = piece[...]
        assert stop <= half


def positions():
    return {axis: lax.axis_index(axis) for axis in ("x", "z", "y", "c")}


def forward_kernel(*refs):
    count = len(CUT_PLACES)
    first, second, refs = refs[:count], refs[count : 2 * count], refs[2 * count :]
    wbs, refs = refs[:4], refs[4:]
    flags, pars, branch, n_all, w_all, keep, val, res = refs
    blocks, steps, _, wide = keep.shape
    half = steps * ROWS
    here = positions()
    for k, dz in enumerate(FIRST + SECOND):
        w_all[k] = wbs[dz][...].reshape(w_all.shape[1:])
    middle = n_all.shape[2] // 2
    pack(first, here, n_all, slice(0, middle))
    pack(second, here, n_all, slice(middle, 2 * middle))
    for m in range(blocks):
        fill_keep(m, flags[m], pars, keep)
    model = n_all.shape[2]
    got = jnp.dot(
        n_all[...].reshape(blocks * half, model),
        w_all[...].reshape(model, 2 * wide),
        preferred_element_type=F32,
    )
    val[0] = got[:, :wide].reshape(blocks, steps, ROWS, wide)
    val[1] = got[:, wide:].reshape(blocks, steps, ROWS, wide)
    both_ways(False, 2, pars, keep, val, res)
    c_re, c_im = pars[3:4, :], pars[4:5, :]
    for m in range(blocks):
        s_re = res[0, m].reshape(half, wide)
        s_im = res[1, m].reshape(half, wide)
        branch[m, :, :wide] = (c_re * s_re - c_im * s_im).astype(BF16)
        branch[m, :, wide:] = (c_re * s_im + c_im * s_re).astype(BF16)


def outer_kernel(*refs):
    pieces, refs = refs[: len(CUT_PLACES)], refs[len(CUT_PLACES) :]
    ig, outs, n_cut = refs[0], refs[1:-1], refs[-1]
    blocks, half, _ = n_cut.shape
    pack(pieces, positions(), n_cut)
    across = outs[0].shape[1]
    for k, out in enumerate(outs):
        rows = n_cut[:, :, k * across : (k + 1) * across].reshape(blocks * half, across)
        out[...] = jnp.dot(ig[...], rows, preferred_element_type=F32).astype(out.dtype)


def flipped(here, place):
    x, y, c = (here[axis] ^ bit for axis, bit in zip(SLAB, place))
    return (x * 2 + y) * 2 + c, x, y * 2 + c


def pre_kernel(own, other, out):
    out[...] = own[...] + other[...].astype(F32)


def sum_kernel(count, *refs):
    sent, outs, held = refs[:count], refs[count:-count - 2], refs[-count - 2 : -2]
    total, done = refs[-2:]
    copies = [pltpu.make_async_copy(src, dst, done.at[k]) for k, (src, dst) in enumerate(zip(sent, held))]
    for copy in copies:
        copy.start()
    for copy in copies:
        copy.wait()
    _, rows, wide = outs[0].shape
    got = held[0][...]
    for other in held[1:]:
        got = got + other[...].astype(F32)
    total[...] = got
    here = positions()
    for k, place in enumerate(PLACES):
        _, part, d = flipped(here, place)
        at = pl.ds(pl.multiple_of(part * wide, wide), wide)
        columns = pl.ds(pl.multiple_of(d * rows, rows), rows)
        outs[place[2]][k % 4] = total[at, columns].T.astype(BF16)


def pair_kernel(same, came, *outs):
    for k, out in enumerate(outs):
        out[0] = same[k]
        out[1] = came[k]


def place_kernel(*refs):
    got, out = refs[:-1], refs[-1]
    here = positions()
    for (dx, dy, dc), block in zip(PLACES, [block.at[c] for c in (0, 1) for block in got]):
        m, _, _ = flipped(here, (dx, dy, dc))
        wide = block.shape[1]
        out[:, pl.ds(pl.multiple_of(m * wide, wide), wide)] = block[...].astype(F32)


def mixed_kernel(tokens, gain, skip, branch, out):
    members, half, both = branch.shape
    wide = both // 2
    widened, normed = rms_rows(tokens[0], gain[...])
    base = widened + skip[...] * normed.astype(F32)
    back = reorder(half, True)
    for m in range(members):
        got = jnp.dot(back, branch[m], preferred_element_type=F32)
        for part in range(2):
            columns = slice((part * members + m) * wide, (part * members + m + 1) * wide)
            total = base[:, columns] + got[:, part * wide : (part + 1) * wide]
            out[0, :, columns] = total.astype(BF16)


def call(kernel, out_shape, inputs, scratch=(), mib=8, flops=1_000_000, spaces=None):
    vmem = pl.BlockSpec(memory_space=pltpu.VMEM)
    made = jax.tree.leaves(out_shape)
    moved = sum(a.size * a.dtype.itemsize for a in [*inputs, *made])
    return pl.pallas_call(
        kernel,
        out_shape=out_shape,
        in_specs=[pl.BlockSpec(memory_space=space) for space in spaces or [pltpu.VMEM] * len(inputs)],
        out_specs=jax.tree.map(lambda _: vmem, out_shape),
        scratch_shapes=list(scratch),
        compiler_params=pltpu.CompilerParams(vmem_limit_bytes=mib * 2**20),
        cost_estimate=pl.CostEstimate(flops=flops, bytes_accessed=moved, transcendentals=0),
    )(*inputs)


def body_slab(layout, *inputs):
    return slab_step(layout, *inputs)


def slab_step(layout, tokens, token_ids, norm_gain, w_in, rates, phases, forget, readout, skip, out_grad):
    half, model = tokens.shape[1:]
    pairs = rates.shape[0]
    n_z, count = layout["z"], PIECES
    members = 2 * count
    wide = pairs // members
    steps = half // ROWS
    mine = (lax.axis_index("x") * 2 + lax.axis_index("y")) * 2 + lax.axis_index("c")

    def shaped(shape, dtype=BF16):
        return jax.ShapeDtypeStruct(shape, dtype)

    w_cut = call(cut_kernel, [shaped((w_in.shape[0], 2 * wide))] * count, [w_in])
    w_cut = list(w_cut)
    w_cut[1] = flip(w_cut[1], "c")
    w_cut[2] = flip(w_cut[2], "y")
    w_cut[3] = flip(w_cut[3], "y", "c")
    w_own = call(stack_kernel, shaped((count, w_in.shape[0], 2 * wide)), w_cut)
    w_2 = z_flip(w_own, 2, n_z)
    w_1 = z_flip(w_own, 1, n_z)
    w_3 = z_flip(w_2, 1, n_z)

    gain = norm_gain.reshape(1, model)
    first, second = call(
        norm_kernel,
        [shaped((half, model // 2))] * 2,
        [tokens, gain],
        [pltpu.VMEM(tokens.shape, BF16), pltpu.VMEM((half, model), BF16), pltpu.SemaphoreType.DMA],
        spaces=[pl.ANY, pltpu.VMEM],
    )
    first = [first, flip(first, "x"), flip(first, "y")]
    halves = [shaped((half // 2, model // 2))] * 2
    top, bottom = call(halve_kernel, halves, [first[2], first[1]])
    first += [flip(top, "x"), flip(bottom, "y")]
    second = [second, flip(second, "x"), flip(second, "y")]
    top, bottom = call(halve_kernel, halves, [second[2], second[1]])
    second += [flip(top, "x"), flip(bottom, "y")]
    first += [flip(piece, "c") for piece in first]
    second += [flip(piece, "c") for piece in second]

    under = 16
    og = call(grad_kernel, shaped((members, half + under, 2 * wide)), [out_grad, token_ids])
    og = exchange(og, SLAB)

    radius = jnp.exp(-rates)
    in_scale = jnp.sqrt(-jnp.expm1(-2.0 * rates))
    rows = [radius * jnp.cos(phases), radius * jnp.sin(phases), forget, in_scale * readout[0], in_scale * readout[1]]
    rows = jnp.stack(rows + [jnp.zeros_like(rates)] * (ROWS - len(rows)))
    pars = lax.dynamic_slice_in_dim(rows, mine * wide, wide, axis=1)

    chains = [
        pltpu.VMEM((members, steps, ROWS, wide), F32),
        pltpu.VMEM((2, members, steps, ROWS, wide), F32),
        pltpu.VMEM((2, members, steps, ROWS, wide), F32),
    ]
    ig, flags = call(
        adjoint_kernel,
        [shaped((2 * wide, members * half)), shaped((members, ROWS, wide), F32)],
        [og, pars],
        chains,
        flops=20_000_000,
    )

    across = model // n_z
    matmul = 2 * members * half * model * 2 * wide
    parts = {}
    for pieces, distances in ((first, FIRST), (second, SECOND)):
        made = call(
            outer_kernel,
            [shaped((2 * wide, across), BF16 if dz else F32) for dz in distances],
            [*pieces, ig],
            [pltpu.VMEM((members, half, model // 2), BF16)],
            mib=16,
            flops=matmul // 2,
        )
        parts.update(zip(distances, made))
    got = [z_flip(parts[dz], dz, n_z) for dz in (3, 2, 1)]

    branch = call(
        forward_kernel,
        shaped((members, half, 2 * wide)),
        [*first, *second, w_own, w_1, w_2, w_3, flags, pars],
        [pltpu.VMEM((members, half, model), BF16), pltpu.VMEM((n_z, model // n_z, 2 * wide), BF16)] + chains,
        mib=24,
        flops=matmul,
    )
    branch = exchange(branch, SLAB)
    mixed = call(
        mixed_kernel, shaped(tokens.shape), [tokens, gain, skip.reshape(1, model), branch], flops=10_000_000
    )

    early = call(pre_kernel, shaped((2 * wide, across), F32), [parts[0], got[0]])
    sums = [early, *got[1:]]
    total = call(
        functools.partial(sum_kernel, len(sums)),
        [shaped((count, across // count, wide))] * 2,
        sums,
        [
            *(pltpu.VMEM(part.shape, part.dtype) for part in sums),
            pltpu.VMEM((2 * wide, across), F32),
            pltpu.SemaphoreType.DMA((len(sums),)),
        ],
        mib=8,
        spaces=[pl.ANY] * len(sums),
    )
    same, other = total
    came = flip(other, "c")
    pairs_of = call(pair_kernel, [shaped((2, across // count, wide))] * count, [same, came])
    placed = [
        pairs_of[0], flip(pairs_of[1], "x"), flip(pairs_of[2], "y"), flip(pairs_of[3], "x", "y")
    ]
    grad_w_in = call(place_kernel, shaped((across // count, pairs), F32), placed)
    return (mixed, grad_w_in)


def solution(mesh):
    n_seq, n_fsdp = mesh.shape["seq"], mesh.shape["fsdp"]
    if n_seq == 2 and n_fsdp == 16:
        layout = {"x": n_seq, "z": n_fsdp // 4, "y": 2, "c": 2}
        mesh = Mesh(mesh.devices.reshape(tuple(layout.values())), tuple(layout))
        body, fsdp, seq = functools.partial(body_slab, layout), ("z", "y", "c"), "x"
    else:
        body, fsdp, seq = body_any, "fsdp", "seq"
    in_specs = (
        P(fsdp, seq, None),
        P(fsdp, seq),
        P(),
        P(fsdp, None),
        P(),
        P(),
        P(),
        P(),
        P(),
        P(fsdp, seq, None),
    )
    out_specs = (P(fsdp, seq, None), P(fsdp, seq))
    step = jax.shard_map(body, mesh=mesh, in_specs=in_specs, out_specs=out_specs, check_vma=False)
    if body is body_any:
        return step
    return step
```
